128 devices in a mesh: row: 16 (over y, x), col: 8 (over z, core).
Axes of the slice: x: 4, y: 4, z: 4, core: 2. Of those that a mesh axis runs over, the one named last changes fastest.
Arguments:
- phase: float32 [8192, 4096], P('row', 'col'), may hold values from -1 to 1
- tile_mask: int32 [32, 16], P('row', 'col'), may hold values 0 or 1
Outputs:
- updated: float32 [8192, 4096], P('row', 'col')
- section: float32 [8192, 4096], P('row', 'col')
The draws below stay inside these ranges and needn't reach their ends.
All inputs are finite; a program needn't handle non-finite values. No bound on the sum of `tile_mask` on one device may be relied on, other than what follows from the above.
Results may differ from the reference program's by a relative error of at most 0.0003.
Values sent between devices are 32-bit elements; how exact they have to be, the bound alone decides.
No kernel may reach another device: no remote copies, remote signals or barrier semaphores. Data moves between devices by JAX's collectives and lax.ppermute only.
A program may use at most 64 MiB of HBM per device.

```python
import jax
import jax.numpy as jnp
from jax import lax

TILE = 256
KRYLOV = 3
MROWS = 32
MCOLS = 16
NX = 8192
NY = 4096


def touch_ends(result, own_key, low, largest):
    index_at = [jax.random.randint(jax.random.fold_in(own_key, axis), (), 0, length) for axis, length in enumerate(result.shape)]
    widest = result.shape.index(max(result.shape))
    beside = index_at[:widest] + [(index_at[widest] + 1) % result.shape[widest]] + index_at[widest + 1:]
    return result.at[tuple(index_at)].set(low).at[tuple(beside)].set(largest)


def steps_of(own_key, shape, split, low, high):
    def one(position, parts):
        steps = jax.random.uniform(jax.random.fold_in(jax.random.fold_in(own_key, 6), position), (parts,), jnp.float32, low / len(split), high / len(split))
        return jnp.repeat(jnp.exp(steps), shape[position] // parts).reshape((-1,) + (1,) * (len(shape) - position - 1))

    loudness = one(*split[0])
    for cut in split[1:]:
        loudness = loudness * one(*cut)
    return loudness


def setup_inputs(seed: int = 0) -> dict:
    key_list = jax.random.split(jax.random.key(seed), 3)
    return {
        "phase": jnp.clip(jax.random.uniform(key_list[0], (NX, NY), jnp.float32, -1.0, 1.0) * steps_of(key_list[0], (NX, NY), ((0, 16), (1, 8)), -0.4, 0.0), -1.0, 1.0),
        "tile_mask": touch_ends((jax.random.randint(key_list[1], (MROWS, MCOLS), 0, 4) < 3).astype(jnp.int32), jax.random.fold_in(key_list[1], 1), 0, 1),
    }


diffusion = 2.0
remainder_weight = 32.0

def laplace(field):
    padded = jnp.pad(field, 1)
    return padded[2:, 1:-1] + padded[:-2, 1:-1] + padded[1:-1, 2:] + padded[1:-1, :-2] - 4.0 * field

def operate(field, coef, active):
    return active * (diffusion * laplace(field) + coef * field)

def exponential(matrix):
    size = matrix.shape[0]
    eye = jnp.eye(size, dtype=jnp.float32)
    scaled = matrix * (1.0 / 1024.0)
    term = eye
    total = eye
    for degree in range(1, 11):
        term = jnp.dot(term, scaled, precision=lax.Precision.HIGHEST) / float(degree)
        total = total + term
    for squaring in range(10):
        total = jnp.dot(total, total, precision=lax.Precision.HIGHEST)
    return total

def phi_column(hess, scale, order):
    width = hess.shape[0]
    size = width + order
    augmented = jnp.zeros((size, size), jnp.float32)
    augmented = augmented.at[:width, :width].set(scale * hess)
    augmented = augmented.at[0, width].set(1.0)
    for offset in range(order - 1):
        augmented = augmented.at[width + offset, width + offset + 1].set(1.0)
    return exponential(augmented)[:width, size - 1]

def arnoldi(start, coef, active):
    beta = jnp.sqrt(jnp.sum(start * start))
    basis = [start / beta]
    hess = jnp.zeros((KRYLOV, KRYLOV), jnp.float32)
    for column in range(KRYLOV):
        image = operate(basis[column], coef, active)
        coeffs = jnp.stack([jnp.sum(vector * image) for vector in basis])
        hess = hess.at[:column + 1, column].set(coeffs)
        if column + 1 < KRYLOV:
            rest = image
            for index_k in range(column + 1):
                rest = rest - coeffs[index_k] * basis[index_k]
            length = jnp.sqrt(jnp.sum(rest * rest))
            hess = hess.at[column + 1, column].set(length)
            basis.append(rest / length)
    return (beta, basis, hess)

def combine(beta, basis, weights):
    total = jnp.zeros_like(basis[0])
    for index_k in range(len(basis)):
        total = total + weights[index_k] * basis[index_k]
    return beta * total

def reference(phase, tile_mask):
    masks = tile_mask.astype(jnp.float32)
    active = jnp.repeat(jnp.repeat(masks, TILE, axis=0), TILE, axis=1)
    force = operate(phase, 1.0 - phase * phase, active)
    slope = 1.0 - 3.0 * phase * phase
    beta_one, basis_one, hess_one = arnoldi(force, slope, active)
    shift = 0.5 * combine(beta_one, basis_one, phi_column(hess_one, 0.5, 1))
    section = phase + shift
    remainder = -active * shift * shift * (shift + 3.0 * phase)
    beta_two, basis_two, hess_two = arnoldi(remainder, slope, active)
    first = combine(beta_one, basis_one, phi_column(hess_one, 1.0, 1))
    third = combine(beta_two, basis_two, phi_column(hess_two, 1.0, 3))
    updated = phase + first + remainder_weight * third
    return (updated, section)
```

```python
import functools

import jax
import jax.numpy as jnp
from jax import lax
from jax.experimental import pallas as pl
from jax.experimental.pallas import tpu as pltpu
from jax.sharding import Mesh
from jax.sharding import PartitionSpec as P

TILE = 256
ROW = ("row_0", "row_1")
COL = ("col_0", "col_1")
ALL = ROW + COL
HALO = 8
LANES = 128
UNROLL = 4


def splat(row, lane, k):
    return jnp.broadcast_to(
        jnp.sum(jnp.where(lane == k, row, 0.0), axis=1, keepdims=True), (8, LANES)
    )


def matmul3(a, b):
    return [
        [a[i][0] * b[0][j] + a[i][1] * b[1][j] + a[i][2] * b[2][j] for j in range(3)]
        for i in range(3)
    ]


def phi_column(hess, scale, order):
    inv = 1.0 / 1024.0
    base = [[hess[i][j] * (scale * inv) for j in range(3)] for i in range(3)]
    zero = jnp.zeros((8, LANES), jnp.float32)
    term = base
    cols = [[zero + inv, zero, zero]] + [[zero] * 3 for _ in range(order - 1)]
    total = base
    sums = cols
    for degree in range(2, 11):
        first = [term[i][0] * (inv / degree) for i in range(3)]
        cols = [first] + [[c * (inv / degree) for c in col] for col in cols[:-1]]
        term = [[v * (1.0 / degree) for v in row] for row in matmul3(term, base)]
        total = [[total[i][j] + term[i][j] for j in range(3)] for i in range(3)]
        sums = [[s + c for s, c in zip(sc, cc)] for sc, cc in zip(sums, cols)]
    one, two = inv, 0.5 * inv * inv
    for _ in range(10):
        moved = []
        for n, col in enumerate(sums):
            new = [
                2.0 * col[i]
                + (total[i][0] * col[0] + total[i][1] * col[1] + total[i][2] * col[2])
                for i in range(3)
            ]
            if n >= 1:
                new = [new[i] + sums[n - 1][i] * one for i in range(3)]
            if n >= 2:
                new = [new[i] + sums[n - 2][i] * two for i in range(3)]
            moved.append(new)
        square = matmul3(total, total)
        total = [[2.0 * total[i][j] + square[i][j] for j in range(3)] for i in range(3)]
        sums = moved
        one, two = 2.0 * one, 2.0 * two + one * one
    return sums[-1]


def hessenberg(gathered):
    lane = lax.broadcasted_iota(jnp.int32, (8, LANES), 1)
    row = jnp.broadcast_to(jnp.sum(gathered, axis=0, keepdims=True), (8, LANES))
    g = {}
    for n, (i, j) in enumerate(PAIRS):
        g[i, j] = splat(row, lane, n)
    r = {}
    r[0, 0] = jnp.sqrt(g[0, 0])
    for m in (1, 2, 3):
        r[0, m] = g[0, m] / r[0, 0]
    r[1, 1] = jnp.sqrt(jnp.maximum(g[1, 1] - r[0, 1] * r[0, 1], 1e-9 * g[1, 1]))
    for m in (2, 3):
        r[1, m] = (g[1, m] - r[0, 1] * r[0, m]) / r[1, 1]
    r[2, 2] = jnp.sqrt(
        jnp.maximum(g[2, 2] - r[0, 2] * r[0, 2] - r[1, 2] * r[1, 2], 1e-9 * g[2, 2])
    )
    r[2, 3] = (g[2, 3] - r[0, 2] * r[0, 3] - r[1, 2] * r[1, 3]) / r[2, 2]
    zero = jnp.zeros((8, LANES), jnp.float32)
    c0 = [8.0 * r[0, 1] / r[0, 0], 8.0 * r[1, 1] / r[0, 0], zero]
    c1 = [(8.0 * r[0, 2] - c0[0] * r[0, 1]) / r[1, 1], (8.0 * r[1, 2] - c0[1] * r[0, 1]) / r[1, 1], 8.0 * r[2, 2] / r[1, 1]]
    c2 = [
        (8.0 * r[0, 3] - c0[0] * r[0, 2] - c1[0] * r[1, 2]) / r[2, 2],
        (8.0 * r[1, 3] - c0[1] * r[0, 2] - c1[1] * r[1, 2]) / r[2, 2],
        (8.0 * r[2, 3] - c1[2] * r[1, 2]) / r[2, 2],
    ]
    hess = [[c0[i], c1[i], c2[i]] for i in range(3)]
    for i in range(3):
        hess[i][i] = hess[i][i] - 8.0
    return r, hess


PAIRS = tuple((i, j) for i in range(3) for j in range(i, 4))


def on_basis(r, weights, factor):
    scale = factor * r[0, 0]
    d2 = weights[2] / r[2, 2]
    d1 = (weights[1] - r[1, 2] * d2) / r[1, 1]
    d0 = (weights[0] - r[0, 1] * d1 - r[0, 2] * d2) / r[0, 0]
    return [d0 * scale, d1 * scale, d2 * scale]


def around(ref, at):
    tiles = ref.shape[0]
    lane = lax.broadcasted_iota(jnp.int32, (8, LANES), 1)
    mids = [ref[j, pl.ds(at, 8), :] for j in range(tiles)]
    ones = [pltpu.roll(m, 1, 1) for m in mids]
    backs = [pltpu.roll(m, LANES - 1, 1) for m in mids]
    out = []
    for j in range(tiles):
        left = jnp.where(lane == 0, ones[j - 1], ones[j])
        right = jnp.where(lane == LANES - 1, backs[(j + 1) % tiles], backs[j])
        rows = ref[j, pl.ds(at - 1, 8), :] + ref[j, pl.ds(at + 1, 8), :]
        out.append((left + right) + rows)
    return mids, out


def write_sums(sums, out_ref):
    lane = lax.broadcasted_iota(jnp.int32, (1, LANES), 1)
    row = jnp.zeros((1, LANES), jnp.float32)
    for n, s in enumerate(sums):
        row = row + jnp.where(lane == n, jnp.sum(s), 0.0)
    out_ref[...] = jnp.broadcast_to(row, out_ref.shape)


def for_bands(n, body, init=0, halo=True):
    count = n // TILE
    carry = init
    if halo:
        carry = body(8, 0, carry)
    for t in range(count):

        def group(i, c, t=t):
            at = 16 + t * TILE + i * (8 * UNROLL)
            for u in range(UNROLL):
                c = body(at + 8 * u, t + 1, c)
            return c

        carry = lax.fori_loop(0, TILE // (8 * UNROLL), group, carry)
    if halo:
        carry = body(n + 16, count + 1, carry)
    return carry


def act_of(act_ref, band):
    return [act_ref[j, band : band + 1, :] for j in range(act_ref.shape[0])]


def powers_and_sums(fields, coef_ref, act_ref, n):
    w0, w1, w2 = fields
    tiles = w0.shape[0]

    def apply(src, dst):
        def body(at, band, c):
            mids, sides = around(src, at)
            for j, act in enumerate(act_of(act_ref, band)):
                dst[j, pl.ds(at, 8), :] = (0.25 * act) * sides[j] + coef_ref[j, pl.ds(at, 8), :] * mids[j]
            return c

        return body

    for_bands(n, apply(w0, w1))
    for_bands(n, apply(w1, w2))

    def last(at, band, sums):
        mids, sides = around(w2, at)
        acts = act_of(act_ref, band)
        sums = list(sums)
        for j in range(tiles - 1):
            here = pl.ds(at, 8)
            third = (0.25 * acts[j]) * sides[j] + coef_ref[j, here, :] * mids[j]
            basis = [w0[j, here, :], w1[j, here, :], mids[j], third]
            for k, (a, b) in enumerate(PAIRS):
                sums[k] = sums[k] + basis[a] * basis[b]
        return tuple(sums)

    zero = jnp.zeros((8, LANES), jnp.float32)
    return for_bands(n, last, tuple(zero for _ in PAIRS), halo=False)


def strips_kernel(left_ref, right_ref, mask_ref, to_left_ref, to_right_ref):
    n = left_ref.shape[0]
    lane = lax.broadcasted_iota(jnp.int32, (8, LANES), 1)
    for ref, out, rows, col in ((left_ref, to_left_ref, 0, 0), (right_ref, to_right_ref, 120, mask_ref.shape[1] - 1)):
        out[:, :n] = ref[...].T[rows : rows + 8, :]
        extra = jnp.zeros((8, LANES), jnp.float32)
        for t in range(mask_ref.shape[0]):
            extra = extra + jnp.where(lane == t, mask_ref[t, col].astype(jnp.float32), 0.0)
        out[:, n:] = extra


def corners_kernel(from_left_ref, from_right_ref, top_ref, bottom_ref, mask_ref, side_ref, up_ref, down_ref):
    n = side_ref.shape[0]
    width = top_ref.shape[1]
    tiles_r, tiles_c = mask_ref.shape
    zeros = jnp.zeros((LANES - 16, n), jnp.float32)
    side = jnp.concatenate([from_right_ref[:, :n], zeros, from_left_ref[:, :n]], axis=0).T
    side_ref[...] = side
    lane = lax.broadcasted_iota(jnp.int32, (8, LANES), 1)
    from_left = from_left_ref[:, n:]
    from_right = from_right_ref[:, n:]
    for ref, out, rows, t in ((top_ref, up_ref, 0, 0), (bottom_ref, down_ref, n - 8, tiles_r - 1)):
        out[:, :width] = ref[...]
        extra = side[rows : rows + 8, :]
        for c in range(tiles_c):
            extra = jnp.where(lane == 16 + c, mask_ref[t, c].astype(jnp.float32), extra)
        extra = jnp.where(lane == 16 + tiles_c, splat(from_right, lane, t), extra)
        extra = jnp.where(lane == 17 + tiles_c, splat(from_left, lane, t), extra)
        out[:, width:] = extra


def first_kernel(
    phase_ref, side_ref, up_ref, down_ref, from_left_ref, from_right_ref, mask_ref,
    p_ref, w0, w1, w2, coef_ref, act_ref, sums_ref,
):
    n, width = phase_ref.shape
    tiles = p_ref.shape[0]
    tiles_r, tiles_c = mask_ref.shape
    lane = lax.broadcasted_iota(jnp.int32, (8, LANES), 1)

    def cells(band, values, right, left):
        for j in range(tiles - 1):
            act_ref[j, band : band + 1, :] = jnp.full((1, LANES), values[j * LANES // TILE])
        ends = jnp.where(lane < 8, right, jnp.where(lane >= LANES - 8, left, 0.0))
        act_ref[tiles - 1, band : band + 1, :] = ends[0:1]

    def pick(ref, at, k):
        return jnp.sum(jnp.where(lane == k, ref[:, at:], 0.0)[0:1, :])

    for t, ref in ((0, up_ref), (tiles_r + 1, down_ref)):
        values = [pick(ref, width, 16 + c) for c in range(tiles_c + 2)]
        cells(t, values[:tiles_c], values[tiles_c], values[tiles_c + 1])
    for t in range(tiles_r):
        values = [mask_ref[t, c].astype(jnp.float32) for c in range(tiles_c)]
        cells(t + 1, values, pick(from_right_ref, n, t), pick(from_left_ref, n, t))

    blank = jnp.zeros((8, LANES), jnp.float32)
    for ref in (p_ref, w0, w1, w2):
        for j in range(tiles):
            ref[j, 0:8, :] = blank
            ref[j, n + 24 : n + 32, :] = blank
    for at, ref in ((8, up_ref), (n + 16, down_ref)):
        for j in range(tiles - 1):
            p_ref[j, at : at + 8, :] = ref[:, j * LANES : (j + 1) * LANES]
        p_ref[tiles - 1, at : at + 8, :] = jnp.where((lane < 8) | (lane >= LANES - 8), ref[:, width:], 0.0)
    for j in range(tiles - 1):
        p_ref[j, 16 : n + 16, :] = phase_ref[:, j * LANES : (j + 1) * LANES]
    p_ref[tiles - 1, 16 : n + 16, :] = side_ref[...]

    def force(at, band, c):
        mids, sides = around(p_ref, at)
        for j, act in enumerate(act_of(act_ref, band)):
            square = mids[j] * mids[j]
            w0[j, pl.ds(at, 8), :] = act * (2.0 * sides[j] - (7.0 + square) * mids[j])
            coef_ref[j, pl.ds(at, 8), :] = act * (0.125 - 0.375 * square)
        return c

    for_bands(n, force)
    write_sums(powers_and_sums((w0, w1, w2), coef_ref, act_ref, n), sums_ref)


def second_kernel(
    gathered_ref, p_ref, w0, w1, w2, coef_ref, act_ref,
    section_ref, base_ref, v0, v1, v2, sums_ref,
):
    n, width = section_ref.shape
    tiles = p_ref.shape[0]
    r, hess = hessenberg(gathered_ref[...])
    lane = lax.broadcasted_iota(jnp.int32, (8, LANES), 1)
    half = lane < LANES // 2
    scale = jnp.where(half, 0.5, 1.0)
    weights = phi_column(hess, scale, 1)
    coefs = on_basis(r, weights, scale)
    a = [jnp.max(jnp.where(half, c, -jnp.inf)) for c in coefs]
    f = [jnp.max(jnp.where(half, -jnp.inf, c)) for c in coefs]
    blank = jnp.zeros((8, LANES), jnp.float32)
    for ref in (v0, v1, v2):
        for j in range(tiles):
            ref[j, 0:8, :] = blank
            ref[j, n + 24 : n + 32, :] = blank

    def start(at, band, c):
        acts = act_of(act_ref, band)
        here = pl.ds(at, 8)
        for j in range(tiles):
            ws = [ref[j, here, :] for ref in (w0, w1, w2)]
            phase = p_ref[j, here, :]
            shift = a[0] * ws[0] + a[1] * ws[1] + a[2] * ws[2]
            v0[j, here, :] = -acts[j] * (shift * shift) * (shift + 3.0 * phase)
            if j < tiles - 1 and 1 <= band <= n // TILE:
                to = pl.ds(pl.multiple_of(at - 16, 8), 8)
                cols = slice(j * LANES, (j + 1) * LANES)
                first = f[0] * ws[0] + f[1] * ws[1] + f[2] * ws[2]
                section_ref[to, cols] = phase + shift
                base_ref[to, cols] = phase + first
        return c

    for_bands(n, start)
    write_sums(powers_and_sums((v0, v1, v2), coef_ref, act_ref, n), sums_ref)


def third_kernel(gathered_ref, base_ref, v0, v1, v2, updated_ref):
    n, width = base_ref.shape
    r, hess = hessenberg(gathered_ref[...])
    coefs = on_basis(r, phi_column(hess, 1.0, 3), 32.0)
    d = [jnp.max(c) for c in coefs]

    def body(at, band, c):
        to = pl.ds(pl.multiple_of(at - 16, 8), 8)
        for j in range(width // LANES):
            vs = [ref[j, pl.ds(at, 8), :] for ref in (v0, v1, v2)]
            cols = slice(j * LANES, (j + 1) * LANES)
            updated_ref[to, cols] = base_ref[to, cols] + (d[0] * vs[0] + d[1] * vs[1] + d[2] * vs[2])
        return c

    for_bands(n, body, halo=False)


def params(mib):
    return pltpu.CompilerParams(vmem_limit_bytes=mib << 20)


VM = pl.BlockSpec(memory_space=pltpu.VMEM)
SM = pl.BlockSpec(memory_space=pltpu.SMEM)


def both_ways(low, high, axis):
    size = lax.axis_size(axis)
    up = [(i, i + 1) for i in range(size - 1)]
    return lax.ppermute(high, axis, up), lax.ppermute(low, axis, [(b, a) for a, b in up])


def total(sums):
    size = sums.shape[0]
    sent = lax.all_to_all(sums.reshape(size, 1, LANES), ALL, 0, 0, tiled=True)
    return sent.reshape(size, LANES)


def body(phase, tile_mask):
    n, width = phase.shape
    f32 = jnp.float32
    sd = jax.ShapeDtypeStruct
    to_left, to_right = pl.pallas_call(
        strips_kernel,
        grid=(1,),
        in_specs=[
            pl.BlockSpec((n, LANES), lambda i: (0, 0)),
            pl.BlockSpec((n, LANES), lambda i: (0, width // LANES - 1)),
            SM,
        ],
        out_shape=[sd((8, n + LANES), f32)] * 2,
        compiler_params=params(4),
        name="strips",
    )(phase, phase, tile_mask)
    from_left, from_right = both_ways(to_left, to_right, COL)
    side, to_up, to_down = pl.pallas_call(
        corners_kernel,
        in_specs=[VM] * 4 + [SM],
        out_shape=[sd((n, LANES), f32)] + [sd((8, width + LANES), f32)] * 2,
        compiler_params=params(4),
        name="corners",
    )(from_left, from_right, phase[:8], phase[n - 8 :], tile_mask)
    from_up, from_down = both_ways(to_up, to_down, ROW)
    devices = 1
    for axis in ALL:
        devices *= lax.axis_size(axis)
    tiles = width // LANES + 1
    ext = sd((tiles, n + 32, LANES), f32)
    act = sd((tiles, 8, LANES), f32)
    sums = sd((devices, LANES), f32)
    p, w0, w1, w2, coef, act, part = pl.pallas_call(
        first_kernel,
        in_specs=[VM] * 6 + [SM],
        out_specs=[VM] * 7,
        out_shape=[ext, ext, ext, ext, ext, act, sums],
        compiler_params=params(20),
        name="first",
    )(phase, side, from_up, from_down, from_left, from_right, tile_mask)
    own = sd((n, width), f32)
    section, base, v0, v1, v2, part = pl.pallas_call(
        second_kernel,
        in_specs=[VM] * 7,
        out_specs=[VM] * 6,
        out_shape=[own, own, ext, ext, ext, sums],
        compiler_params=params(24),
        name="second",
    )(total(part), p, w0, w1, w2, coef, act)
    updated = pl.pallas_call(
        third_kernel,
        in_specs=[VM] * 5,
        out_specs=VM,
        out_shape=own,
        compiler_params=params(12),
        name="third",
    )(total(part), base, v0, v1, v2)
    return updated, section


def solution(mesh):
    split = Mesh(mesh.devices.reshape(4, 4, 4, 2), ALL)
    in_specs = (P(ROW, COL), P(ROW, COL))
    out_specs = (P(ROW, COL), P(ROW, COL))
    return jax.shard_map(body, mesh=split, in_specs=in_specs, out_specs=out_specs, check_vma=False)
```

```python
import functools

import jax
import jax.numpy as jnp
from jax import lax
from jax.experimental import pallas as pl
from jax.experimental.pallas import tpu as pltpu
from jax.sharding import Mesh
from jax.sharding import PartitionSpec as P

TILE = 256
ROW = ("row_0", "row_1")
COL = ("col_0", "col_1")
ALL = ROW + COL
HALO = 8
LANES = 128
UNROLL = 11


def splat(row, lane, k):
    return jnp.broadcast_to(
        jnp.sum(jnp.where(lane == k, row, 0.0), axis=1, keepdims=True), (8, LANES)
    )


def matmul3(a, b):
    return [
        [a[i][0] * b[0][j] + a[i][1] * b[1][j] + a[i][2] * b[2][j] for j in range(3)]
        for i in range(3)
    ]


def phi_column(hess, scale, order):
    inv = 1.0 / 1024.0
    base = [[hess[i][j] * (scale * inv) for j in range(3)] for i in range(3)]
    zero = jnp.zeros((8, LANES), jnp.float32)
    term = base
    cols = [[zero + inv, zero, zero]] + [[zero] * 3 for _ in range(order - 1)]
    total = base
    sums = cols
    for degree in range(2, 11):
        first = [term[i][0] * (inv / degree) for i in range(3)]
        cols = [first] + [[c * (inv / degree) for c in col] for col in cols[:-1]]
        term = [[v * (1.0 / degree) for v in row] for row in matmul3(term, base)]
        total = [[total[i][j] + term[i][j] for j in range(3)] for i in range(3)]
        sums = [[s + c for s, c in zip(sc, cc)] for sc, cc in zip(sums, cols)]
    one, two = inv, 0.5 * inv * inv
    for _ in range(10):
        moved = []
        for n, col in enumerate(sums):
            new = [
                2.0 * col[i]
                + (total[i][0] * col[0] + total[i][1] * col[1] + total[i][2] * col[2])
                for i in range(3)
            ]
            if n >= 1:
                new = [new[i] + sums[n - 1][i] * one for i in range(3)]
            if n >= 2:
                new = [new[i] + sums[n - 2][i] * two for i in range(3)]
            moved.append(new)
        square = matmul3(total, total)
        total = [[2.0 * total[i][j] + square[i][j] for j in range(3)] for i in range(3)]
        sums = moved
        one, two = 2.0 * one, 2.0 * two + one * one
    return sums[-1]


def hessenberg(gathered):
    lane = lax.broadcasted_iota(jnp.int32, (8, LANES), 1)
    row = jnp.broadcast_to(jnp.sum(gathered, axis=0, keepdims=True), (8, LANES))
    moments = [splat(row, lane, n) for n in range(6)]
    g = {(i, j): moments[i + j] for i in range(3) for j in range(i, 4)}
    r = {}
    r[0, 0] = jnp.sqrt(g[0, 0])
    for m in (1, 2, 3):
        r[0, m] = g[0, m] / r[0, 0]
    r[1, 1] = jnp.sqrt(jnp.maximum(g[1, 1] - r[0, 1] * r[0, 1], 1e-9 * g[1, 1]))
    for m in (2, 3):
        r[1, m] = (g[1, m] - r[0, 1] * r[0, m]) / r[1, 1]
    r[2, 2] = jnp.sqrt(
        jnp.maximum(g[2, 2] - r[0, 2] * r[0, 2] - r[1, 2] * r[1, 2], 1e-9 * g[2, 2])
    )
    r[2, 3] = (g[2, 3] - r[0, 2] * r[0, 3] - r[1, 2] * r[1, 3]) / r[2, 2]
    zero = jnp.zeros((8, LANES), jnp.float32)
    c0 = [8.0 * r[0, 1] / r[0, 0], 8.0 * r[1, 1] / r[0, 0], zero]
    c1 = [(8.0 * r[0, 2] - c0[0] * r[0, 1]) / r[1, 1], (8.0 * r[1, 2] - c0[1] * r[0, 1]) / r[1, 1], 8.0 * r[2, 2] / r[1, 1]]
    c2 = [
        (8.0 * r[0, 3] - c0[0] * r[0, 2] - c1[0] * r[1, 2]) / r[2, 2],
        (8.0 * r[1, 3] - c0[1] * r[0, 2] - c1[1] * r[1, 2]) / r[2, 2],
        (8.0 * r[2, 3] - c1[2] * r[1, 2]) / r[2, 2],
    ]
    hess = [[c0[i], c1[i], c2[i]] for i in range(3)]
    for i in range(3):
        hess[i][i] = hess[i][i] - 8.0
    return r, hess


def on_basis(r, weights, factor):
    scale = factor * r[0, 0]
    d2 = weights[2] / r[2, 2]
    d1 = (weights[1] - r[1, 2] * d2) / r[1, 1]
    d0 = (weights[0] - r[0, 1] * d1 - r[0, 2] * d2) / r[0, 0]
    return [d0 * scale, d1 * scale, d2 * scale]


def beside(ref, at, sides):
    tiles = ref.shape[0]
    lane = lax.broadcasted_iota(jnp.int32, (8, LANES), 1)
    mids = [ref[j, pl.ds(at, 8), :] for j in range(tiles)]
    ones = [pltpu.roll(m, 1, 1) for m in mids]
    out = [jnp.where(lane == 0, ones[j - 1], ones[j]) for j in range(tiles)]
    if sides == 2:
        backs = [pltpu.roll(m, LANES - 1, 1) for m in mids]
        out = [o + jnp.where(lane == LANES - 1, backs[(j + 1) % tiles], backs[j]) for j, o in enumerate(out)]
    return out


def write_sums(sums, out_ref):
    lane = lax.broadcasted_iota(jnp.int32, (1, LANES), 1)
    row = jnp.zeros((1, LANES), jnp.float32)
    for n, tiles in enumerate(sums):
        row = row + jnp.where(lane == n, jnp.sum(sum(tiles[1:], tiles[0])), 0.0)
    out_ref[...] = jnp.broadcast_to(row, out_ref.shape)


def band_of(group, bands):
    return jnp.clip((group - 1 + TILE // 8) // (TILE // 8), 0, bands - 1)


def act_of(act_ref, group):
    band = pl.multiple_of(8 * band_of(group, act_ref.shape[1] // 8), 8)
    return [act_ref[j, pl.ds(band, 8), :] for j in range(act_ref.shape[0])]


def stencil_pass(src, side_ref, groups, first, emit, carry, sides=2):
    unroll = UNROLL
    while groups % unroll:
        unroll -= 1
    steps = groups // unroll

    def ahead(group, at):
        for u in range(unroll):
            for j, v in enumerate(beside(src, at + 8 * u, sides)):
                side_ref[j, pl.ds(at + 8 * u, 8), :] = v

    def here(group, at, c):
        for u in range(unroll):
            side = [side_ref[j, pl.ds(at + 8 * u, 8), :] for j in range(src.shape[0])]
            c = emit(group + u, at + 8 * u, side, u, c)
        return c

    def both(i, c):
        group = first + i * unroll
        at = pl.multiple_of(8 + 8 * group, 8)
        c = here(group, at, c)
        ahead(group + unroll, at + 8 * unroll)
        return c

    ahead(first, 8 + 8 * first)
    carry = lax.fori_loop(0, steps - 1, both, carry)
    group = first + (steps - 1) * unroll
    return here(group, 8 + 8 * group, carry)


def add_products(sums, pairs, own):
    out = []
    for row, (a, b) in zip(sums, pairs):
        new = []
        for j, s in enumerate(row):
            product = a[j] * b[j]
            new.append(s + (product if own is None else product * own))
        out.append(tuple(new))
    return tuple(out)


def own_of(group, groups, u, unroll):
    if 0 < u < unroll - 1:
        return None
    return jnp.where((group > 0) & (group < groups - 1), 1.0, 0.0)


def no_sums(count, tiles):
    return tuple(tuple(jnp.zeros((8, LANES), jnp.float32) for _ in range(tiles - 1)) for _ in range(count))


def powers(fields, coef_ref, act_ref, side_ref):
    w0, w1, w2 = fields
    tiles = w0.shape[0]
    groups = (w0.shape[1] - 16) // 8

    def apply(src, dst):
        def emit(group, at, side, u, sums):
            acts = act_of(act_ref, group)
            here = pl.ds(at, 8)
            mids, outs = [], []
            for j in range(tiles):
                mid = src[j, here, :]
                total = side[j] + (src[j, pl.ds(at - 1, 8), :] + src[j, pl.ds(at + 1, 8), :])
                out = acts[j] * total + coef_ref[j, here, :] * mid
                dst[j, here, :] = out
                mids.append(mid)
                outs.append(out)
            own = own_of(group, groups, u, UNROLL)
            return add_products(sums, ((mids, outs), (outs, outs)), own)

        return stencil_pass(src, side_ref, groups, 0, emit, no_sums(2, tiles))

    m1, m2 = apply(w0, w1)
    m3, m4 = apply(w1, w2)

    def emit(group, at, side, u, sums):
        here = pl.ds(at, 8)
        mids, images = [], []
        for j in range(tiles - 1):
            mid = w2[j, here, :]
            images.append(0.5 * (side[j] + w2[j, pl.ds(at - 1, 8), :]) + coef_ref[j, here, :] * mid)
            mids.append(mid)
        return add_products(sums, ((mids, images),), None)

    (m5,) = stencil_pass(w2, side_ref, groups - 2, 1, emit, no_sums(1, tiles), sides=1)
    return [m1, m2, m3, m4, m5]


def strips_kernel(odd_ref, phase_hbm, mask_hbm, near_ref, far_ref, left_ref, right_ref, mask_ref, sems):
    n, width = phase_hbm.shape
    copies = [
        pltpu.make_async_copy(phase_hbm.at[:, 0:LANES], left_ref, sems.at[0]),
        pltpu.make_async_copy(phase_hbm.at[:, width - LANES : width], right_ref, sems.at[1]),
        pltpu.make_async_copy(mask_hbm, mask_ref, sems.at[2]),
    ]
    for c in copies:
        c.start()
    for c in copies:
        c.wait()
    odd = jnp.full((8, LANES), odd_ref[1], jnp.int32) > 0
    odd_n = jnp.full((8, n), odd_ref[1], jnp.int32) > 0
    lane = lax.broadcasted_iota(jnp.int32, (8, LANES), 1)
    strips = []
    for ref, rows, col in ((left_ref, 0, 0), (right_ref, LANES - 8, mask_ref.shape[1] - 1)):
        extra = jnp.zeros((8, LANES), jnp.float32)
        for t in range(mask_ref.shape[0]):
            extra = extra + jnp.where(lane == t, mask_ref[t, col].astype(jnp.float32), 0.0)
        strips.append((ref[...].T[rows : rows + 8, :], extra))
    left, right = strips
    for out, a, b in ((near_ref, left, right), (far_ref, right, left)):
        out[:, :n] = jnp.where(odd_n, a[0], b[0])
        out[:, n:] = jnp.where(odd, a[1], b[1])


def corners_kernel(odd_ref, near_in, far_in, phase_ref, mask_ref, side_ref, near_ref, far_ref, masks_ref):
    n, width = phase_ref.shape
    tiles_r, tiles_c = mask_ref.shape
    odd = jnp.full((8, LANES), odd_ref[1], jnp.int32) > 0
    odd_n = jnp.full((8, n), odd_ref[1], jnp.int32) > 0
    from_left = jnp.where(odd_n, near_in[:, :n], far_in[:, :n])
    from_right = jnp.where(odd_n, far_in[:, :n], near_in[:, :n])
    mask_left = jnp.where(odd, near_in[:, n:], far_in[:, n:])
    mask_right = jnp.where(odd, far_in[:, n:], near_in[:, n:])
    masks_ref[0] = mask_left
    masks_ref[1] = mask_right
    zeros = jnp.zeros((LANES - 16, n), jnp.float32)
    side = jnp.concatenate([from_right, zeros, from_left], axis=0).T
    side_ref[...] = side
    lane = lax.broadcasted_iota(jnp.int32, (8, LANES), 1)
    strips = []
    for rows, t in ((0, 0), (n - 8, tiles_r - 1)):
        extra = side[rows : rows + 8, :]
        for c in range(tiles_c):
            extra = jnp.where(lane == 16 + c, mask_ref[t, c].astype(jnp.float32), extra)
        extra = jnp.where(lane == 16 + tiles_c, splat(mask_right, lane, t), extra)
        extra = jnp.where(lane == 17 + tiles_c, splat(mask_left, lane, t), extra)
        strips.append((phase_ref[rows : rows + 8, :], extra))
    up, down = strips
    odd = jnp.full((8, LANES), odd_ref[0], jnp.int32) > 0
    odd_w = jnp.full((8, width), odd_ref[0], jnp.int32) > 0
    for out, a, b in ((near_ref, up, down), (far_ref, down, up)):
        out[:, :width] = jnp.where(odd_w, a[0], b[0])
        out[:, width:] = jnp.where(odd, a[1], b[1])


def first_kernel(
    odd_ref, phase_ref, side_in, near_in, far_in, masks_ref, mask_ref,
    p_ref, w0, w1, w2, coef_ref, act_ref, sums_ref, side_ref,
):
    n, width = phase_ref.shape
    tiles = p_ref.shape[0]
    groups = n // 8 + 2
    tiles_r, tiles_c = mask_ref.shape
    lane = lax.broadcasted_iota(jnp.int32, (8, LANES), 1)
    odd = jnp.full((8, LANES), odd_ref[0], jnp.int32) > 0
    up = [jnp.where(odd, near_in[:, j * LANES : (j + 1) * LANES], far_in[:, j * LANES : (j + 1) * LANES]) for j in range(tiles)]
    down = [jnp.where(odd, far_in[:, j * LANES : (j + 1) * LANES], near_in[:, j * LANES : (j + 1) * LANES]) for j in range(tiles)]

    def cells(band, values, right, left):
        for j in range(tiles - 1):
            act_ref[j, 8 * band : 8 * band + 8, :] = 0.25 * jnp.broadcast_to(values[j * LANES // TILE], (8, LANES))
        ends = jnp.where(lane < 8, right, jnp.where(lane >= LANES - 8, left, 0.0))
        act_ref[tiles - 1, 8 * band : 8 * band + 8, :] = 0.25 * ends

    for t, extra in ((0, up[-1]), (tiles_r + 1, down[-1])):
        values = [splat(extra, lane, 16 + c) for c in range(tiles_c + 2)]
        cells(t, values[:tiles_c], values[tiles_c], values[tiles_c + 1])
    for t in range(tiles_r):
        values = [mask_ref[t, c].astype(jnp.float32) for c in range(tiles_c)]
        cells(t + 1, values, splat(masks_ref[1], lane, t), splat(masks_ref[0], lane, t))

    blank = jnp.zeros((8, LANES), jnp.float32)
    for ref in (p_ref, w0, w1, w2):
        for j in range(tiles):
            ref[j, 0:8, :] = blank
            ref[j, n + 24 : n + 32, :] = blank
    for at, rows in ((8, up), (n + 16, down)):
        for j in range(tiles - 1):
            p_ref[j, at : at + 8, :] = rows[j]
        p_ref[tiles - 1, at : at + 8, :] = jnp.where((lane < 8) | (lane >= LANES - 8), rows[-1], 0.0)
    for j in range(tiles - 1):
        p_ref[j, 16 : n + 16, :] = phase_ref[:, j * LANES : (j + 1) * LANES]
    p_ref[tiles - 1, 16 : n + 16, :] = side_in[...]

    def force(group, at, side, u, sums):
        acts = act_of(act_ref, group)
        here = pl.ds(at, 8)
        outs = []
        for j in range(tiles):
            mid = p_ref[j, here, :]
            total = side[j] + (p_ref[j, pl.ds(at - 1, 8), :] + p_ref[j, pl.ds(at + 1, 8), :])
            square = mid * mid
            out = acts[j] * (8.0 * total - (28.0 + 4.0 * square) * mid)
            w0[j, here, :] = out
            coef_ref[j, here, :] = acts[j] * (0.5 - 1.5 * square)
            outs.append(out)
        return add_products(sums, ((outs, outs),), own_of(group, groups, u, UNROLL))

    (m0,) = stencil_pass(p_ref, side_ref, groups, 0, force, no_sums(1, tiles))
    write_sums([m0] + powers((w0, w1, w2), coef_ref, act_ref, side_ref), sums_ref)


def second_kernel(
    gathered_ref, p_ref, w0, w1, w2, coef_ref, act_ref,
    section_ref, base_ref, v0, v1, v2, sums_ref, side_ref,
):
    n, width = section_ref.shape
    tiles = p_ref.shape[0]
    r, hess = hessenberg(gathered_ref[...])
    lane = lax.broadcasted_iota(jnp.int32, (8, LANES), 1)
    half = lane < LANES // 2
    scale = jnp.where(half, 0.5, 1.0)
    weights = phi_column(hess, scale, 1)
    coefs = on_basis(r, weights, scale)
    a = [jnp.max(jnp.where(half, c, -jnp.inf)) for c in coefs]
    f = [jnp.max(jnp.where(half, -jnp.inf, c)) for c in coefs]
    blank = jnp.zeros((8, LANES), jnp.float32)
    for ref in (v0, v1, v2):
        for j in range(tiles):
            ref[j, 0:8, :] = blank
            ref[j, n + 24 : n + 32, :] = blank

    def start(group, own, sums):
        at = pl.multiple_of(8 + 8 * group, 8)
        acts = act_of(act_ref, group)
        here = pl.ds(at, 8)
        outs = []
        for j in range(tiles):
            ws = [ref[j, here, :] for ref in (w0, w1, w2)]
            phase = p_ref[j, here, :]
            shift = a[0] * ws[0] + a[1] * ws[1] + a[2] * ws[2]
            out = (-4.0 * acts[j]) * (shift * shift) * (shift + 3.0 * phase)
            v0[j, here, :] = out
            outs.append(out)
            if j < tiles - 1 and own:
                to = pl.ds(pl.multiple_of(at - 16, 8), 8)
                cols = slice(j * LANES, (j + 1) * LANES)
                first = f[0] * ws[0] + f[1] * ws[1] + f[2] * ws[2]
                section_ref[to, cols] = phase + shift
                base_ref[to, cols] = phase + first
        return add_products(sums, ((outs, outs),), None) if own else sums

    def four(i, sums):
        for u in range(4):
            sums = start(1 + 4 * i + u, True, sums)
        return sums

    start(0, False, None)
    (m0,) = lax.fori_loop(0, n // 32, four, no_sums(1, tiles))
    start(n // 8 + 1, False, None)
    write_sums([m0] + powers((v0, v1, v2), coef_ref, act_ref, side_ref), sums_ref)


def third_kernel(gathered_ref, base_ref, v0, v1, v2, updated_ref):
    n, width = base_ref.shape
    r, hess = hessenberg(gathered_ref[...])
    coefs = on_basis(r, phi_column(hess, 1.0, 3), 32.0)
    d = [jnp.max(c) for c in coefs]

    def four(i, c):
        for u in range(4):
            at = pl.multiple_of(32 * i, 8) + 8 * u
            for j in range(width // LANES):
                vs = [ref[j, pl.ds(at + 16, 8), :] for ref in (v0, v1, v2)]
                cols = slice(j * LANES, (j + 1) * LANES)
                updated_ref[pl.ds(at, 8), cols] = base_ref[pl.ds(at, 8), cols] + (
                    d[0] * vs[0] + d[1] * vs[1] + d[2] * vs[2]
                )
        return c

    lax.fori_loop(0, n // 32, four, 0)


def params(mib):
    return pltpu.CompilerParams(vmem_limit_bytes=mib << 20)


VM = pl.BlockSpec(memory_space=pltpu.VMEM)
SM = pl.BlockSpec(memory_space=pltpu.SMEM)
HB = pl.BlockSpec(memory_space=pltpu.HBM)


def in_pairs(near, far, axis):
    size = lax.axis_size(axis)
    odd = [(i, ((i + 1) ^ 1) - 1) for i in range(1, size - 1)]
    return lax.ppermute(near, axis, [(i, i ^ 1) for i in range(size)]), lax.ppermute(far, axis, odd)


def total(sums):
    size = sums.shape[0]
    sent = lax.all_to_all(sums.reshape(size, 1, LANES), ALL, 0, 0, tiled=True)
    return sent.reshape(size, LANES)


def body(phase, tile_mask):
    n, width = phase.shape
    f32 = jnp.float32
    sd = jax.ShapeDtypeStruct
    odd = jnp.stack([lax.axis_index(ROW) % 2, lax.axis_index(COL) % 2]).astype(jnp.int32)
    edge = sd((8, width + LANES), f32)
    near, far = pl.pallas_call(
        strips_kernel,
        in_specs=[SM, HB, HB],
        out_specs=[VM] * 2,
        out_shape=[sd((8, n + LANES), f32)] * 2,
        scratch_shapes=[
            pltpu.VMEM((n, LANES), f32),
            pltpu.VMEM((n, LANES), f32),
            pltpu.SMEM(tile_mask.shape, jnp.int32),
            pltpu.SemaphoreType.DMA((3,)),
        ],
        compiler_params=params(4),
        name="strips",
    )(odd, phase, tile_mask)
    near, far = in_pairs(near, far, COL)
    side, near, far, masks = pl.pallas_call(
        corners_kernel,
        in_specs=[SM, VM, VM, VM, SM],
        out_specs=[VM] * 4,
        out_shape=[sd((n, LANES), f32), edge, edge, sd((2, 8, LANES), f32)],
        compiler_params=params(6),
        name="corners",
    )(odd, near, far, phase, tile_mask)
    near, far = in_pairs(near, far, ROW)
    devices = 1
    for axis in ALL:
        devices *= lax.axis_size(axis)
    tiles = width // LANES + 1
    ext = sd((tiles, n + 32, LANES), f32)
    act = sd((tiles, 8 * (tile_mask.shape[0] + 2), LANES), f32)
    scratch = [pltpu.VMEM((tiles, n + 32, LANES), f32)]
    sums = sd((devices, LANES), f32)
    p, w0, w1, w2, coef, act, part = pl.pallas_call(
        first_kernel,
        in_specs=[SM] + [VM] * 5 + [SM],
        out_specs=[VM] * 7,
        scratch_shapes=scratch,
        out_shape=[ext, ext, ext, ext, ext, act, sums],
        compiler_params=params(22),
        name="first",
    )(odd, phase, side, near, far, masks, tile_mask)
    own = sd((n, width), f32)
    section, base, v0, v1, v2, part = pl.pallas_call(
        second_kernel,
        in_specs=[VM] * 7,
        out_specs=[VM] * 6,
        scratch_shapes=scratch,
        out_shape=[own, own, ext, ext, ext, sums],
        compiler_params=params(26),
        name="second",
    )(total(part), p, w0, w1, w2, coef, act)
    updated = pl.pallas_call(
        third_kernel,
        in_specs=[VM] * 5,
        out_specs=VM,
        out_shape=own,
        compiler_params=params(12),
        name="third",
    )(total(part), base, v0, v1, v2)
    return updated, section


def solution(mesh):
    split = Mesh(mesh.devices.reshape(4, 4, 4, 2), ALL)
    in_specs = (P(ROW, COL), P(ROW, COL))
    out_specs = (P(ROW, COL), P(ROW, COL))
    return jax.shard_map(body, mesh=split, in_specs=in_specs, out_specs=out_specs, check_vma=False)
```

```python
import functools

import jax
import jax.numpy as jnp
from jax import lax
from jax.experimental import pallas as pl
from jax.experimental.pallas import tpu as pltpu
from jax.sharding import Mesh
from jax.sharding import PartitionSpec as P

TILE = 256
ROW = ("row_0", "row_1")
COL = ("col_0", "col_1")
ALL = ROW + COL
HALO = 8
LANES = 128
UNROLL = 33


def splat(row, lane, k):
    return jnp.broadcast_to(
        jnp.sum(jnp.where(lane == k, row, 0.0), axis=1, keepdims=True), (8, LANES)
    )


def matmul3(a, b):
    return [
        [a[i][0] * b[0][j] + a[i][1] * b[1][j] + a[i][2] * b[2][j] for j in range(3)]
        for i in range(3)
    ]


def phi_column(hess, scale, order):
    inv = 1.0 / 1024.0
    base = [[hess[i][j] * (scale * inv) for j in range(3)] for i in range(3)]
    zero = jnp.zeros((8, LANES), jnp.float32)
    term = base
    cols = [[zero + inv, zero, zero]] + [[zero] * 3 for _ in range(order - 1)]
    total = base
    sums = cols
    for degree in range(2, 11):
        first = [term[i][0] * (inv / degree) for i in range(3)]
        cols = [first] + [[c * (inv / degree) for c in col] for col in cols[:-1]]
        term = [[v * (1.0 / degree) for v in row] for row in matmul3(term, base)]
        total = [[total[i][j] + term[i][j] for j in range(3)] for i in range(3)]
        sums = [[s + c for s, c in zip(sc, cc)] for sc, cc in zip(sums, cols)]
    one, two = inv, 0.5 * inv * inv
    for _ in range(10):
        moved = []
        for n, col in enumerate(sums):
            new = [
                2.0 * col[i]
                + (total[i][0] * col[0] + total[i][1] * col[1] + total[i][2] * col[2])
                for i in range(3)
            ]
            if n >= 1:
                new = [new[i] + sums[n - 1][i] * one for i in range(3)]
            if n >= 2:
                new = [new[i] + sums[n - 2][i] * two for i in range(3)]
            moved.append(new)
        square = matmul3(total, total)
        total = [[2.0 * total[i][j] + square[i][j] for j in range(3)] for i in range(3)]
        sums = moved
        one, two = 2.0 * one, 2.0 * two + one * one
    return sums[-1]


def hessenberg(gathered):
    lane = lax.broadcasted_iota(jnp.int32, (8, LANES), 1)
    row = jnp.broadcast_to(jnp.sum(gathered, axis=0, keepdims=True), (8, LANES))
    moments = [splat(row, lane, n) for n in range(6)]
    g = {(i, j): moments[i + j] for i in range(3) for j in range(i, 4)}
    r = {}
    r[0, 0] = jnp.sqrt(g[0, 0])
    for m in (1, 2, 3):
        r[0, m] = g[0, m] / r[0, 0]
    r[1, 1] = jnp.sqrt(jnp.maximum(g[1, 1] - r[0, 1] * r[0, 1], 1e-9 * g[1, 1]))
    for m in (2, 3):
        r[1, m] = (g[1, m] - r[0, 1] * r[0, m]) / r[1, 1]
    r[2, 2] = jnp.sqrt(
        jnp.maximum(g[2, 2] - r[0, 2] * r[0, 2] - r[1, 2] * r[1, 2], 1e-9 * g[2, 2])
    )
    r[2, 3] = (g[2, 3] - r[0, 2] * r[0, 3] - r[1, 2] * r[1, 3]) / r[2, 2]
    zero = jnp.zeros((8, LANES), jnp.float32)
    c0 = [8.0 * r[0, 1] / r[0, 0], 8.0 * r[1, 1] / r[0, 0], zero]
    c1 = [(8.0 * r[0, 2] - c0[0] * r[0, 1]) / r[1, 1], (8.0 * r[1, 2] - c0[1] * r[0, 1]) / r[1, 1], 8.0 * r[2, 2] / r[1, 1]]
    c2 = [
        (8.0 * r[0, 3] - c0[0] * r[0, 2] - c1[0] * r[1, 2]) / r[2, 2],
        (8.0 * r[1, 3] - c0[1] * r[0, 2] - c1[1] * r[1, 2]) / r[2, 2],
        (8.0 * r[2, 3] - c1[2] * r[1, 2]) / r[2, 2],
    ]
    hess = [[c0[i], c1[i], c2[i]] for i in range(3)]
    for i in range(3):
        hess[i][i] = hess[i][i] - 8.0
    return r, hess


def on_basis(r, weights, factor):
    scale = factor * r[0, 0]
    d2 = weights[2] / r[2, 2]
    d1 = (weights[1] - r[1, 2] * d2) / r[1, 1]
    d0 = (weights[0] - r[0, 1] * d1 - r[0, 2] * d2) / r[0, 0]
    return [d0 * scale, d1 * scale, d2 * scale]


def beside(ref, at, sides):
    tiles = ref.shape[0]
    lane = lax.broadcasted_iota(jnp.int32, (8, LANES), 1)
    mids = [ref[j, pl.ds(at, 8), :] for j in range(tiles)]
    ones = [pltpu.roll(m, 1, 1) for m in mids]
    out = [jnp.where(lane == 0, ones[j - 1], ones[j]) for j in range(tiles)]
    if sides == 2:
        backs = [pltpu.roll(m, LANES - 1, 1) for m in mids]
        out = [o + jnp.where(lane == LANES - 1, backs[(j + 1) % tiles], backs[j]) for j, o in enumerate(out)]
    return out


def write_sums(sums, out_ref):
    lane = lax.broadcasted_iota(jnp.int32, (1, LANES), 1)
    row = jnp.zeros((1, LANES), jnp.float32)
    for n, tiles in enumerate(sums):
        row = row + jnp.where(lane == n, jnp.sum(sum(tiles[1:], tiles[0])), 0.0)
    out_ref[...] = jnp.broadcast_to(row, out_ref.shape)


def band_of(group, bands):
    return jnp.clip((group - 1 + TILE // 8) // (TILE // 8), 0, bands - 1)


def act_of(act_ref, group):
    band = pl.multiple_of(8 * band_of(group, act_ref.shape[1] // 8), 8)
    return [act_ref[j, pl.ds(band, 8), :] for j in range(act_ref.shape[0])]


def stencil_pass(src, side_ref, groups, first, emit, carry, sides=2):
    unroll = UNROLL
    while groups % unroll:
        unroll -= 1
    steps = groups // unroll

    def step(i, c):
        group = first + i * unroll
        at = pl.multiple_of(8 + 8 * group, 8)
        for u in range(unroll):
            c = emit(group + u, at + 8 * u, beside(src, at + 8 * u, sides), u, c)
        return c

    return lax.fori_loop(0, steps, step, carry)


def add_products(sums, pairs, own):
    out = []
    for row, (a, b) in zip(sums, pairs):
        new = []
        for j, s in enumerate(row):
            product = a[j] * b[j]
            new.append(s + (product if own is None else product * own))
        out.append(tuple(new))
    return tuple(out)


def own_of(group, groups, u, unroll):
    if 0 < u < unroll - 1:
        return None
    return jnp.where((group > 0) & (group < groups - 1), 1.0, 0.0)


def no_sums(count, tiles):
    return tuple(tuple(jnp.zeros((8, LANES), jnp.float32) for _ in range(tiles - 1)) for _ in range(count))


def powers(fields, coef_ref, act_ref, side_ref):
    w0, w1, w2 = fields
    tiles = w0.shape[0]
    groups = (w0.shape[1] - 16) // 8

    def apply(src, dst):
        def emit(group, at, side, u, sums):
            acts = act_of(act_ref, group)
            here = pl.ds(at, 8)
            mids, outs = [], []
            for j in range(tiles):
                mid = src[j, here, :]
                total = side[j] + (src[j, pl.ds(at - 1, 8), :] + src[j, pl.ds(at + 1, 8), :])
                out = acts[j] * total + coef_ref[j, here, :] * mid
                dst[j, here, :] = out
                mids.append(mid)
                outs.append(out)
            own = own_of(group, groups, u, UNROLL)
            return add_products(sums, ((mids, outs), (outs, outs)), own)

        return stencil_pass(src, side_ref, groups, 0, emit, no_sums(2, tiles))

    m1, m2 = apply(w0, w1)
    m3, m4 = apply(w1, w2)

    def emit(group, at, side, u, sums):
        here = pl.ds(at, 8)
        mids, images = [], []
        for j in range(tiles - 1):
            mid = w2[j, here, :]
            images.append(0.5 * (side[j] + w2[j, pl.ds(at - 1, 8), :]) + coef_ref[j, here, :] * mid)
            mids.append(mid)
        return add_products(sums, ((mids, images),), None)

    (m5,) = stencil_pass(w2, side_ref, groups - 2, 1, emit, no_sums(1, tiles), sides=1)
    return [m1, m2, m3, m4, m5]


def strips_kernel(odd_ref, phase_hbm, mask_hbm, near_ref, far_ref, left_ref, right_ref, mask_ref, sems):
    n, width = phase_hbm.shape
    copies = [
        pltpu.make_async_copy(phase_hbm.at[:, 0:LANES], left_ref, sems.at[0]),
        pltpu.make_async_copy(phase_hbm.at[:, width - LANES : width], right_ref, sems.at[1]),
        pltpu.make_async_copy(mask_hbm, mask_ref, sems.at[2]),
    ]
    for c in copies:
        c.start()
    for c in copies:
        c.wait()
    odd = jnp.full((8, LANES), odd_ref[1], jnp.int32) > 0
    odd_n = jnp.full((8, n), odd_ref[1], jnp.int32) > 0
    lane = lax.broadcasted_iota(jnp.int32, (8, LANES), 1)
    strips = []
    for ref, rows, col in ((left_ref, 0, 0), (right_ref, LANES - 8, mask_ref.shape[1] - 1)):
        extra = jnp.zeros((8, LANES), jnp.float32)
        for t in range(mask_ref.shape[0]):
            extra = extra + jnp.where(lane == t, mask_ref[t, col].astype(jnp.float32), 0.0)
        strips.append((ref[...].T[rows : rows + 8, :], extra))
    left, right = strips
    for out, a, b in ((near_ref, left, right), (far_ref, right, left)):
        out[:, :n] = jnp.where(odd_n, a[0], b[0])
        out[:, n:] = jnp.where(odd, a[1], b[1])


def corners_kernel(odd_ref, near_in, far_in, phase_ref, mask_ref, side_ref, near_ref, far_ref, masks_ref):
    n, width = phase_ref.shape
    tiles_r, tiles_c = mask_ref.shape
    odd = jnp.full((8, LANES), odd_ref[1], jnp.int32) > 0
    odd_n = jnp.full((8, n), odd_ref[1], jnp.int32) > 0
    from_left = jnp.where(odd_n, near_in[:, :n], far_in[:, :n])
    from_right = jnp.where(odd_n, far_in[:, :n], near_in[:, :n])
    mask_left = jnp.where(odd, near_in[:, n:], far_in[:, n:])
    mask_right = jnp.where(odd, far_in[:, n:], near_in[:, n:])
    masks_ref[0] = mask_left
    masks_ref[1] = mask_right
    zeros = jnp.zeros((LANES - 16, n), jnp.float32)
    side = jnp.concatenate([from_right, zeros, from_left], axis=0).T
    side_ref[...] = side
    lane = lax.broadcasted_iota(jnp.int32, (8, LANES), 1)
    strips = []
    for rows, t in ((0, 0), (n - 8, tiles_r - 1)):
        extra = side[rows : rows + 8, :]
        for c in range(tiles_c):
            extra = jnp.where(lane == 16 + c, mask_ref[t, c].astype(jnp.float32), extra)
        extra = jnp.where(lane == 16 + tiles_c, splat(mask_right, lane, t), extra)
        extra = jnp.where(lane == 17 + tiles_c, splat(mask_left, lane, t), extra)
        strips.append((phase_ref[rows : rows + 8, :], extra))
    up, down = strips
    odd = jnp.full((8, LANES), odd_ref[0], jnp.int32) > 0
    odd_w = jnp.full((8, width), odd_ref[0], jnp.int32) > 0
    for out, a, b in ((near_ref, up, down), (far_ref, down, up)):
        out[:, :width] = jnp.where(odd_w, a[0], b[0])
        out[:, width:] = jnp.where(odd, a[1], b[1])


def first_kernel(
    odd_ref, phase_ref, side_in, near_in, far_in, masks_ref, mask_ref,
    p_ref, w0, w1, w2, coef_ref, act_ref, sums_ref, side_ref,
):
    n, width = phase_ref.shape
    tiles = p_ref.shape[0]
    groups = n // 8 + 2
    tiles_r, tiles_c = mask_ref.shape
    lane = lax.broadcasted_iota(jnp.int32, (8, LANES), 1)
    odd = jnp.full((8, LANES), odd_ref[0], jnp.int32) > 0
    up = [jnp.where(odd, near_in[:, j * LANES : (j + 1) * LANES], far_in[:, j * LANES : (j + 1) * LANES]) for j in range(tiles)]
    down = [jnp.where(odd, far_in[:, j * LANES : (j + 1) * LANES], near_in[:, j * LANES : (j + 1) * LANES]) for j in range(tiles)]

    def cells(band, values, right, left):
        for j in range(tiles - 1):
            act_ref[j, 8 * band : 8 * band + 8, :] = 0.25 * jnp.broadcast_to(values[j * LANES // TILE], (8, LANES))
        ends = jnp.where(lane < 8, right, jnp.where(lane >= LANES - 8, left, 0.0))
        act_ref[tiles - 1, 8 * band : 8 * band + 8, :] = 0.25 * ends

    for t, extra in ((0, up[-1]), (tiles_r + 1, down[-1])):
        values = [splat(extra, lane, 16 + c) for c in range(tiles_c + 2)]
        cells(t, values[:tiles_c], values[tiles_c], values[tiles_c + 1])
    for t in range(tiles_r):
        values = [mask_ref[t, c].astype(jnp.float32) for c in range(tiles_c)]
        cells(t + 1, values, splat(masks_ref[1], lane, t), splat(masks_ref[0], lane, t))

    blank = jnp.zeros((8, LANES), jnp.float32)
    for ref in (p_ref, w0, w1, w2):
        for j in range(tiles):
            ref[j, 0:8, :] = blank
            ref[j, n + 24 : n + 32, :] = blank
    for at, rows in ((8, up), (n + 16, down)):
        for j in range(tiles - 1):
            p_ref[j, at : at + 8, :] = rows[j]
        p_ref[tiles - 1, at : at + 8, :] = jnp.where((lane < 8) | (lane >= LANES - 8), rows[-1], 0.0)
    for j in range(tiles - 1):
        p_ref[j, 16 : n + 16, :] = phase_ref[:, j * LANES : (j + 1) * LANES]
    p_ref[tiles - 1, 16 : n + 16, :] = side_in[...]

    def force(group, at, side, u, sums):
        acts = act_of(act_ref, group)
        here = pl.ds(at, 8)
        outs = []
        for j in range(tiles):
            mid = p_ref[j, here, :]
            total = side[j] + (p_ref[j, pl.ds(at - 1, 8), :] + p_ref[j, pl.ds(at + 1, 8), :])
            square = mid * mid
            out = acts[j] * (8.0 * total - (28.0 + 4.0 * square) * mid)
            w0[j, here, :] = out
            coef_ref[j, here, :] = acts[j] * (0.5 - 1.5 * square)
            outs.append(out)
        return add_products(sums, ((outs, outs),), own_of(group, groups, u, UNROLL))

    (m0,) = stencil_pass(p_ref, side_ref, groups, 0, force, no_sums(1, tiles))
    write_sums([m0] + powers((w0, w1, w2), coef_ref, act_ref, side_ref), sums_ref)


def second_kernel(
    gathered_ref, p_ref, w0, w1, w2, coef_ref, act_ref,
    section_ref, base_ref, v0, v1, v2, sums_ref, side_ref,
):
    n, width = section_ref.shape
    tiles = p_ref.shape[0]
    r, hess = hessenberg(gathered_ref[...])
    lane = lax.broadcasted_iota(jnp.int32, (8, LANES), 1)
    half = lane < LANES // 2
    scale = jnp.where(half, 0.5, 1.0)
    weights = phi_column(hess, scale, 1)
    coefs = on_basis(r, weights, scale)
    a = [jnp.max(jnp.where(half, c, -jnp.inf)) for c in coefs]
    f = [jnp.max(jnp.where(half, -jnp.inf, c)) for c in coefs]
    blank = jnp.zeros((8, LANES), jnp.float32)
    for ref in (v0, v1, v2):
        for j in range(tiles):
            ref[j, 0:8, :] = blank
            ref[j, n + 24 : n + 32, :] = blank

    def start(group, own, sums):
        at = pl.multiple_of(8 + 8 * group, 8)
        acts = act_of(act_ref, group)
        here = pl.ds(at, 8)
        outs = []
        for j in range(tiles):
            ws = [ref[j, here, :] for ref in (w0, w1, w2)]
            phase = p_ref[j, here, :]
            shift = a[0] * ws[0] + a[1] * ws[1] + a[2] * ws[2]
            out = (-4.0 * acts[j]) * (shift * shift) * (shift + 3.0 * phase)
            v0[j, here, :] = out
            outs.append(out)
            if j < tiles - 1 and own:
                to = pl.ds(pl.multiple_of(at - 16, 8), 8)
                cols = slice(j * LANES, (j + 1) * LANES)
                first = f[0] * ws[0] + f[1] * ws[1] + f[2] * ws[2]
                section_ref[to, cols] = phase + shift
                base_ref[to, cols] = phase + first
        return add_products(sums, ((outs, outs),), None) if own else sums

    def four(i, sums):
        for u in range(4):
            sums = start(1 + 4 * i + u, True, sums)
        return sums

    start(0, False, None)
    (m0,) = lax.fori_loop(0, n // 32, four, no_sums(1, tiles))
    start(n // 8 + 1, False, None)
    write_sums([m0] + powers((v0, v1, v2), coef_ref, act_ref, side_ref), sums_ref)


def third_kernel(gathered_ref, base_ref, v0, v1, v2, updated_ref):
    n, width = base_ref.shape
    r, hess = hessenberg(gathered_ref[...])
    coefs = on_basis(r, phi_column(hess, 1.0, 3), 32.0)
    d = [jnp.max(c) for c in coefs]

    def four(i, c):
        for u in range(4):
            at = pl.multiple_of(32 * i, 8) + 8 * u
            for j in range(width // LANES):
                vs = [ref[j, pl.ds(at + 16, 8), :] for ref in (v0, v1, v2)]
                cols = slice(j * LANES, (j + 1) * LANES)
                updated_ref[pl.ds(at, 8), cols] = base_ref[pl.ds(at, 8), cols] + (
                    d[0] * vs[0] + d[1] * vs[1] + d[2] * vs[2]
                )
        return c

    lax.fori_loop(0, n // 32, four, 0)


def params(mib):
    return pltpu.CompilerParams(vmem_limit_bytes=mib << 20)


VM = pl.BlockSpec(memory_space=pltpu.VMEM)
SM = pl.BlockSpec(memory_space=pltpu.SMEM)
HB = pl.BlockSpec(memory_space=pltpu.HBM)


def in_pairs(near, far, axis):
    size = lax.axis_size(axis)
    odd = [(i, ((i + 1) ^ 1) - 1) for i in range(1, size - 1)]
    return lax.ppermute(near, axis, [(i, i ^ 1) for i in range(size)]), lax.ppermute(far, axis, odd)


def total(sums):
    size = sums.shape[0]
    sent = lax.all_to_all(sums.reshape(size, 1, LANES), ALL, 0, 0, tiled=True)
    return sent.reshape(size, LANES)


def body(phase, tile_mask):
    n, width = phase.shape
    f32 = jnp.float32
    sd = jax.ShapeDtypeStruct
    odd = jnp.stack([lax.axis_index(ROW) % 2, lax.axis_index(COL) % 2]).astype(jnp.int32)
    edge = sd((8, width + LANES), f32)
    near, far = pl.pallas_call(
        strips_kernel,
        in_specs=[SM, HB, HB],
        out_specs=[VM] * 2,
        out_shape=[sd((8, n + LANES), f32)] * 2,
        scratch_shapes=[
            pltpu.VMEM((n, LANES), f32),
            pltpu.VMEM((n, LANES), f32),
            pltpu.SMEM(tile_mask.shape, jnp.int32),
            pltpu.SemaphoreType.DMA((3,)),
        ],
        compiler_params=params(4),
        name="strips",
    )(odd, phase, tile_mask)
    near, far = in_pairs(near, far, COL)
    side, near, far, masks = pl.pallas_call(
        corners_kernel,
        in_specs=[SM, VM, VM, VM, SM],
        out_specs=[VM] * 4,
        out_shape=[sd((n, LANES), f32), edge, edge, sd((2, 8, LANES), f32)],
        compiler_params=params(6),
        name="corners",
    )(odd, near, far, phase, tile_mask)
    near, far = in_pairs(near, far, ROW)
    devices = 1
    for axis in ALL:
        devices *= lax.axis_size(axis)
    tiles = width // LANES + 1
    ext = sd((tiles, n + 32, LANES), f32)
    act = sd((tiles, 8 * (tile_mask.shape[0] + 2), LANES), f32)
    scratch = [pltpu.VMEM((tiles, n + 32, LANES), f32)]
    sums = sd((devices, LANES), f32)
    p, w0, w1, w2, coef, act, part = pl.pallas_call(
        first_kernel,
        in_specs=[SM] + [VM] * 5 + [SM],
        out_specs=[VM] * 7,
        scratch_shapes=scratch,
        out_shape=[ext, ext, ext, ext, ext, act, sums],
        compiler_params=params(22),
        name="first",
    )(odd, phase, side, near, far, masks, tile_mask)
    own = sd((n, width), f32)
    section, base, v0, v1, v2, part = pl.pallas_call(
        second_kernel,
        in_specs=[VM] * 7,
        out_specs=[VM] * 6,
        scratch_shapes=scratch,
        out_shape=[own, own, ext, ext, ext, sums],
        compiler_params=params(26),
        name="second",
    )(total(part), p, w0, w1, w2, coef, act)
    updated = pl.pallas_call(
        third_kernel,
        in_specs=[VM] * 5,
        out_specs=VM,
        out_shape=own,
        compiler_params=params(12),
        name="third",
    )(total(part), base, v0, v1, v2)
    return updated, section


def solution(mesh):
    split = Mesh(mesh.devices.reshape(4, 4, 4, 2), ALL)
    in_specs = (P(ROW, COL), P(ROW, COL))
    out_specs = (P(ROW, COL), P(ROW, COL))
    return jax.shard_map(body, mesh=split, in_specs=in_specs, out_specs=out_specs, check_vma=False)
```

```python
import functools

import jax
import jax.numpy as jnp
from jax import lax
from jax.experimental import pallas as pl
from jax.experimental.pallas import tpu as pltpu
from jax.sharding import Mesh
from jax.sharding import PartitionSpec as P

TILE = 256
ROW = ("row_0", "row_1")
COL = ("col_0", "col_1")
ALL = ROW + COL
HALO = 8
LANES = 128
UNROLL = 33
CHUNKS = 4


def splat(row, lane, k):
    return jnp.broadcast_to(
        jnp.sum(jnp.where(lane == k, row, 0.0), axis=1, keepdims=True), (8, LANES)
    )


def matmul3(a, b):
    return [
        [a[i][0] * b[0][j] + a[i][1] * b[1][j] + a[i][2] * b[2][j] for j in range(3)]
        for i in range(3)
    ]


def phi_column(hess, scale, order):
    inv = 1.0 / 1024.0
    base = [[hess[i][j] * (scale * inv) for j in range(3)] for i in range(3)]
    zero = jnp.zeros((8, LANES), jnp.float32)
    term = base
    cols = [[zero + inv, zero, zero]] + [[zero] * 3 for _ in range(order - 1)]
    total = base
    sums = cols
    for degree in range(2, 11):
        first = [term[i][0] * (inv / degree) for i in range(3)]
        cols = [first] + [[c * (inv / degree) for c in col] for col in cols[:-1]]
        term = [[v * (1.0 / degree) for v in row] for row in matmul3(term, base)]
        total = [[total[i][j] + term[i][j] for j in range(3)] for i in range(3)]
        sums = [[s + c for s, c in zip(sc, cc)] for sc, cc in zip(sums, cols)]
    one, two = inv, 0.5 * inv * inv
    for _ in range(10):
        moved = []
        for n, col in enumerate(sums):
            new = [
                2.0 * col[i]
                + (total[i][0] * col[0] + total[i][1] * col[1] + total[i][2] * col[2])
                for i in range(3)
            ]
            if n >= 1:
                new = [new[i] + sums[n - 1][i] * one for i in range(3)]
            if n >= 2:
                new = [new[i] + sums[n - 2][i] * two for i in range(3)]
            moved.append(new)
        square = matmul3(total, total)
        total = [[2.0 * total[i][j] + square[i][j] for j in range(3)] for i in range(3)]
        sums = moved
        one, two = 2.0 * one, 2.0 * two + one * one
    return sums[-1]


def root(x):
    inv = lax.rsqrt(x)
    inv = inv * (1.5 - 0.5 * (x * inv) * inv)
    return x * inv, inv


def hessenberg(gathered):
    lane = lax.broadcasted_iota(jnp.int32, (8, LANES), 1)
    row = jnp.broadcast_to(jnp.sum(gathered, axis=0, keepdims=True), (8, LANES))
    m = [splat(row, lane, n) for n in range(6)]
    r00, i0 = root(m[0])
    r01, r02, r03 = m[1] * i0, m[2] * i0, m[3] * i0
    r11, i1 = root(jnp.maximum(m[2] - r01 * r01, 1e-9 * m[2]))
    r12, r13 = (m[3] - r01 * r02) * i1, (m[4] - r01 * r03) * i1
    r22, i2 = root(jnp.maximum(m[4] - r02 * r02 - r12 * r12, 1e-9 * m[4]))
    r23 = (m[5] - r02 * r03 - r12 * r13) * i2
    zero = jnp.zeros((8, LANES), jnp.float32)
    j0, j1, j2 = 8.0 * i0, 8.0 * i1, 8.0 * i2
    c0 = [r01 * j0, r11 * j0, zero]
    d0, d1 = 0.125 * c0[0], 0.125 * c0[1]
    c1 = [(r02 - d0 * r01) * j1, (r12 - d1 * r01) * j1, r22 * j1]
    e0, e1, e2 = [0.125 * v for v in c1]
    c2 = [(r03 - d0 * r02 - e0 * r12) * j2, (r13 - d1 * r02 - e1 * r12) * j2, (r23 - e2 * r12) * j2]
    hess = [[c0[i], c1[i], c2[i]] for i in range(3)]
    for i in range(3):
        hess[i][i] = hess[i][i] - 8.0
    return (r00, r01, r02, r12, i0, i1, i2), hess


def on_basis(r, weights, factor):
    r00, r01, r02, r12, i0, i1, i2 = r
    scale = factor * r00
    d2 = weights[2] * i2
    d1 = (weights[1] - r12 * d2) * i1
    d0 = (weights[0] - r01 * d1 - r02 * d2) * i0
    return [d0 * scale, d1 * scale, d2 * scale]


def beside(ref, at, sides):
    tiles = ref.shape[0]
    lane = lax.broadcasted_iota(jnp.int32, (8, LANES), 1)
    mids = [ref[j, pl.ds(at, 8), :] for j in range(tiles)]
    ones = [pltpu.roll(m, 1, 1) for m in mids]
    out = [jnp.where(lane == 0, ones[j - 1], ones[j]) for j in range(tiles)]
    if sides == 2:
        backs = [pltpu.roll(m, LANES - 1, 1) for m in mids]
        out = [o + jnp.where(lane == LANES - 1, backs[(j + 1) % tiles], backs[j]) for j, o in enumerate(out)]
    return out


def sum_row(sums):
    sub = lax.broadcasted_iota(jnp.int32, (8, LANES), 0)
    lane = lax.broadcasted_iota(jnp.int32, (8, LANES), 1)
    rows = jnp.zeros((8, LANES), jnp.float32)
    for n, tiles in enumerate(sums):
        part = jnp.sum(sum(tiles[1:], tiles[0]), axis=0, keepdims=True)
        rows = jnp.where(sub == n, part, rows)
    values = jnp.sum(rows, axis=1, keepdims=True)
    row = jnp.sum(jnp.where(lane == sub, values, 0.0), axis=0, keepdims=True)
    return jnp.broadcast_to(row, (8, LANES))


def write_row(row, out_ref):
    for i in range(0, out_ref.shape[0], 8):
        out_ref[i : i + 8, :] = row


def band_of(group, bands):
    return jnp.clip((group - 1 + TILE // 8) // (TILE // 8), 0, bands - 1)


def act_of(act_ref, group):
    bands = act_ref.shape[1] // 8
    if isinstance(group, int):
        band = 8 * min(max((group - 1 + TILE // 8) // (TILE // 8), 0), bands - 1)
    else:
        band = pl.multiple_of(8 * band_of(group, bands), 8)
    return [act_ref[j, pl.ds(band, 8), :] for j in range(act_ref.shape[0])]


def over_groups(lo, hi, emit, carry, most=UNROLL):
    unroll = min(most, hi - lo)
    while (hi - lo) % unroll:
        unroll -= 1

    def step(i, c):
        group = lo + i * unroll
        at = pl.multiple_of(8 + 8 * group, 8)
        for u in range(unroll):
            c = emit(group + u, at + 8 * u, c)
        return c

    if hi - lo == unroll:
        for g in range(lo, hi):
            carry = emit(g, 8 + 8 * g, carry)
        return carry
    return lax.fori_loop(0, (hi - lo) // unroll, step, carry)


def is_own(group, groups):
    return not isinstance(group, int) or 0 < group < groups - 1


def add_products(sums, pairs):
    return tuple(
        tuple(s + a[j] * b[j] for j, s in enumerate(row)) for row, (a, b) in zip(sums, pairs)
    )


def no_sums(count, tiles):
    return tuple(tuple(jnp.zeros((8, LANES), jnp.float32) for _ in range(tiles - 1)) for _ in range(count))


def power_of(src, dst, coef_ref, act_ref):
    tiles, rows, _ = src.shape
    groups = (rows - 16) // 8

    def emit(group, at, sums):
        side = beside(src, at, 2)
        acts = act_of(act_ref, group)
        here = pl.ds(at, 8)
        mids, outs = [], []
        for j in range(tiles):
            mid = src[j, here, :]
            total = side[j] + (src[j, pl.ds(at - 1, 8), :] + src[j, pl.ds(at + 1, 8), :])
            out = acts[j] * total + coef_ref[j, here, :] * mid
            dst[j, here, :] = out
            mids.append(mid)
            outs.append(out)
        return add_products(sums, ((mids, outs), (outs, outs))) if is_own(group, groups) else sums

    return emit


def form_of(src, coef_ref):
    tiles = src.shape[0]

    def emit(group, at, sums):
        side = beside(src, at, 1)
        here = pl.ds(at, 8)
        mids, images = [], []
        for j in range(tiles - 1):
            mid = src[j, here, :]
            images.append(0.5 * (side[j] + src[j, pl.ds(at - 1, 8), :]) + coef_ref[j, here, :] * mid)
            mids.append(mid)
        return add_products(sums, ((mids, images),))

    return emit


def force_of(p_ref, w0, coef_ref, act_ref):
    tiles, rows, _ = p_ref.shape
    groups = (rows - 16) // 8

    def emit(group, at, sums):
        side = beside(p_ref, at, 2)
        acts = act_of(act_ref, group)
        here = pl.ds(at, 8)
        outs = []
        for j in range(tiles):
            mid = p_ref[j, here, :]
            total = side[j] + (p_ref[j, pl.ds(at - 1, 8), :] + p_ref[j, pl.ds(at + 1, 8), :])
            square = mid * mid
            out = acts[j] * (8.0 * total - (28.0 + 4.0 * square) * mid)
            w0[j, here, :] = out
            coef_ref[j, here, :] = acts[j] * (0.5 - 1.5 * square)
            outs.append(out)
        return add_products(sums, ((outs, outs),)) if is_own(group, groups) else sums

    return emit


def strips_kernel(odd_ref, phase_hbm, mask_hbm, near_ref, far_ref, own_ref, left_ref, right_ref, mask_ref, sems):
    n, width = phase_hbm.shape
    copies = [
        pltpu.make_async_copy(phase_hbm.at[:, 0:LANES], left_ref, sems.at[0]),
        pltpu.make_async_copy(phase_hbm.at[:, width - LANES : width], right_ref, sems.at[1]),
        pltpu.make_async_copy(mask_hbm, mask_ref, sems.at[2]),
    ]
    for c in copies:
        c.start()
    for c in copies:
        c.wait()
    odd = jnp.full((8, LANES), odd_ref[1], jnp.int32) > 0
    odd_n = jnp.full((8, n), odd_ref[1], jnp.int32) > 0
    lane = lax.broadcasted_iota(jnp.int32, (8, LANES), 1)
    strips = []
    for ref, rows, col in ((left_ref, 0, 0), (right_ref, LANES - 8, mask_ref.shape[1] - 1)):
        extra = jnp.zeros((8, LANES), jnp.float32)
        for t in range(mask_ref.shape[0]):
            extra = extra + jnp.where(lane == t, mask_ref[t, col].astype(jnp.float32), 0.0)
        strips.append((ref[...].T[rows : rows + 8, :], extra))
    own = jnp.zeros((8, LANES), jnp.float32)
    tiles_r, tiles_c = mask_ref.shape
    for t in range(tiles_r):
        for c in range(tiles_c):
            own = jnp.where(lane == t * tiles_c + c, mask_ref[t, c].astype(jnp.float32), own)
    own_ref[...] = own
    left, right = strips
    for out, a, b in ((near_ref, left, right), (far_ref, right, left)):
        out[:, :n] = jnp.where(odd_n, a[0], b[0])
        out[:, n:] = jnp.where(odd, a[1], b[1])


def corners_kernel(odd_ref, near_in, far_in, phase_ref, own_ref, side_ref, near_ref, far_ref, masks_ref):
    n, width = phase_ref.shape
    tiles_r, tiles_c = n // TILE, width // TILE
    odd = jnp.full((8, LANES), odd_ref[1], jnp.int32) > 0
    odd_n = jnp.full((8, n), odd_ref[1], jnp.int32) > 0
    from_left = jnp.where(odd_n, near_in[:, :n], far_in[:, :n])
    from_right = jnp.where(odd_n, far_in[:, :n], near_in[:, :n])
    mask_left = jnp.where(odd, near_in[:, n:], far_in[:, n:])
    mask_right = jnp.where(odd, far_in[:, n:], near_in[:, n:])
    masks_ref[0] = mask_left
    masks_ref[1] = mask_right
    zeros = jnp.zeros((LANES - 16, n), jnp.float32)
    side = jnp.concatenate([from_right, zeros, from_left], axis=0).T
    side_ref[...] = side
    lane = lax.broadcasted_iota(jnp.int32, (8, LANES), 1)
    strips = []
    for rows, t in ((0, 0), (n - 8, tiles_r - 1)):
        extra = side[rows : rows + 8, :]
        for c in range(tiles_c):
            extra = jnp.where(lane == 16 + c, splat(own_ref[...], lane, t * tiles_c + c), extra)
        extra = jnp.where(lane == 16 + tiles_c, splat(mask_right, lane, t), extra)
        extra = jnp.where(lane == 17 + tiles_c, splat(mask_left, lane, t), extra)
        strips.append((phase_ref[rows : rows + 8, :], extra))
    up, down = strips
    odd = jnp.full((8, LANES), odd_ref[0], jnp.int32) > 0
    odd_w = jnp.full((8, width), odd_ref[0], jnp.int32) > 0
    for out, a, b in ((near_ref, up, down), (far_ref, down, up)):
        out[:, :width] = jnp.where(odd_w, a[0], b[0])
        out[:, width:] = jnp.where(odd, a[1], b[1])


def act_cells(act_ref, band, values, right, left):
    tiles = act_ref.shape[0]
    lane = lax.broadcasted_iota(jnp.int32, (8, LANES), 1)
    for j in range(tiles - 1):
        act_ref[j, 8 * band : 8 * band + 8, :] = 0.25 * values[j * LANES // TILE]
    ends = jnp.where(lane < 8, right, jnp.where(lane >= LANES - 8, left, 0.0))
    act_ref[tiles - 1, 8 * band : 8 * band + 8, :] = 0.25 * ends


def first_passes(p_ref, w0, w1, w2, coef_ref, act_ref):
    return (
        (force_of(p_ref, w0, coef_ref, act_ref), 1),
        (power_of(w0, w1, coef_ref, act_ref), 2),
        (power_of(w1, w2, coef_ref, act_ref), 2),
        (form_of(w2, coef_ref), 1),
    )


def inner_kernel(phase_ref, side_in, masks_ref, own_ref, p_ref, w0, w1, w2, coef_ref, act_ref, sums_ref):
    n, width = phase_ref.shape
    tiles = p_ref.shape[0]
    groups = n // 8 + 2
    tiles_r, tiles_c = n // TILE, width // TILE
    lane = lax.broadcasted_iota(jnp.int32, (8, LANES), 1)
    for t in range(tiles_r):
        values = [splat(own_ref[...], lane, t * tiles_c + c) for c in range(tiles_c)]
        act_cells(act_ref, t + 1, values, splat(masks_ref[1], lane, t), splat(masks_ref[0], lane, t))
    for j in range(tiles - 1):
        p_ref[j, 16 : n + 16, :] = phase_ref[:, j * LANES : (j + 1) * LANES]
    p_ref[tiles - 1, 16 : n + 16, :] = side_in[...]
    sums = []
    for k, (emit, count) in enumerate(first_passes(p_ref, w0, w1, w2, coef_ref, act_ref)):
        sums += over_groups(2 + k, groups - 2 - k, emit, no_sums(count, tiles))
    sums_ref[...] = sum_row(sums)


def outer_kernel(
    odd_ref, near_in, far_in, inner_ref, p_in, w0_in, w1_in, w2_in, coef_in, act_in,
    p_ref, w0, w1, w2, coef_ref, act_ref, sums_ref,
):
    tiles, rows, _ = p_ref.shape
    n = rows - 32
    groups = n // 8 + 2
    width = LANES * (tiles - 1)
    tiles_r, tiles_c = n // TILE, width // TILE
    lane = lax.broadcasted_iota(jnp.int32, (8, LANES), 1)
    odd = jnp.full((8, LANES), odd_ref[0], jnp.int32) > 0
    up = [jnp.where(odd, near_in[:, j * LANES : (j + 1) * LANES], far_in[:, j * LANES : (j + 1) * LANES]) for j in range(tiles)]
    down = [jnp.where(odd, far_in[:, j * LANES : (j + 1) * LANES], near_in[:, j * LANES : (j + 1) * LANES]) for j in range(tiles)]
    for t, extra in ((0, up[-1]), (tiles_r + 1, down[-1])):
        values = [splat(extra, lane, 16 + c) for c in range(tiles_c + 2)]
        act_cells(act_ref, t, values[:tiles_c], values[tiles_c], values[tiles_c + 1])
    blank = jnp.zeros((8, LANES), jnp.float32)
    for ref in (p_ref, w0, w1, w2):
        for j in range(tiles):
            ref[j, 0:8, :] = blank
            ref[j, n + 24 : n + 32, :] = blank
    for at, strip in ((8, up), (n + 16, down)):
        for j in range(tiles - 1):
            p_ref[j, at : at + 8, :] = strip[j]
        p_ref[tiles - 1, at : at + 8, :] = jnp.where((lane < 8) | (lane >= LANES - 8), strip[-1], 0.0)
    sums = []
    for k, (emit, count) in enumerate(first_passes(p_ref, w0, w1, w2, coef_ref, act_ref)):
        own = k == 3
        part = no_sums(count, tiles)
        part = over_groups(1 if own else 0, 2 + k, emit, part)
        sums += over_groups(groups - 2 - k, groups - 1 if own else groups, emit, part)
    write_row(sum_row(sums) + inner_ref[...], sums_ref)


def second_kernel(
    gathered_ref, p_ref, w0, w1, w2, coef_ref, act_ref,
    section_hbm, base_ref, v0, v1, v2, sums_ref, section_ref, sem,
):
    tiles, rows, _ = p_ref.shape
    groups = (rows - 16) // 8
    r, hess = hessenberg(gathered_ref[...])
    a = on_basis(r, phi_column(hess, 0.5, 1), 0.5)
    f = on_basis(r, phi_column(hess, 1.0, 1), 1.0)
    blank = jnp.zeros((8, LANES), jnp.float32)
    for ref in (v0, v1, v2):
        for j in range(tiles):
            ref[j, 0:8, :] = blank
            ref[j, rows - 8 : rows, :] = blank

    def start(group, at, sums):
        acts = act_of(act_ref, group)
        here = pl.ds(at, 8)
        own = is_own(group, groups)
        outs = []
        for j in range(tiles):
            ws = [ref[j, here, :] for ref in (w0, w1, w2)]
            phase = p_ref[j, here, :]
            shift = a[0] * ws[0] + a[1] * ws[1] + a[2] * ws[2]
            out = (-4.0 * acts[j]) * (shift * shift) * (shift + 3.0 * phase)
            v0[j, here, :] = out
            outs.append(out)
            if own and j < tiles - 1:
                to = pl.ds(pl.multiple_of(at - 16, 8), 8)
                cols = slice(j * LANES, (j + 1) * LANES)
                section_ref[to, cols] = phase + shift
                base_ref[to, cols] = phase + (f[0] * ws[0] + f[1] * ws[1] + f[2] * ws[2])
        return add_products(sums, ((outs, outs),)) if own else sums

    def sides(emit, count, most):
        part = over_groups(0, 1, emit, no_sums(count, tiles))
        part = over_groups(1, groups - 1, emit, part, most)
        return over_groups(groups - 1, groups, emit, part)

    sums = [*sides(start, 1, 8)]
    copy = pltpu.make_async_copy(section_ref, section_hbm, sem)
    copy.start()
    sums += sides(power_of(v0, v1, coef_ref, act_ref), 2, UNROLL)
    sums += sides(power_of(v1, v2, coef_ref, act_ref), 2, UNROLL)
    sums += over_groups(1, groups - 1, form_of(v2, coef_ref), no_sums(1, tiles))
    write_row(sum_row(sums), sums_ref)
    copy.wait()


def third_kernel(gathered_ref, base_ref, v0, v1, v2, updated_hbm, updated_ref, sems):
    n, width = base_ref.shape
    r, hess = hessenberg(gathered_ref[...])
    d = on_basis(r, phi_column(hess, 1.0, 3), 32.0)

    def emit(group, at, c):
        here = pl.ds(at, 8)
        to = pl.ds(pl.multiple_of(at - 16, 8), 8)
        for j in range(width // LANES):
            cols = slice(j * LANES, (j + 1) * LANES)
            updated_ref[to, cols] = base_ref[to, cols] + (
                d[0] * v0[j, here, :] + d[1] * v1[j, here, :] + d[2] * v2[j, here, :]
            )
        return c

    copies = []
    chunk = n // CHUNKS
    for k in range(CHUNKS):
        over_groups(1 + k * chunk // 8, 1 + (k + 1) * chunk // 8, emit, 0, 4)
        part = pl.ds(k * chunk, chunk)
        copies.append(pltpu.make_async_copy(updated_ref.at[part, :], updated_hbm.at[part, :], sems.at[k]))
        copies[-1].start()
    for copy in copies:
        copy.wait()


def params(mib):
    return pltpu.CompilerParams(vmem_limit_bytes=mib << 20)


VM = pl.BlockSpec(memory_space=pltpu.VMEM)
SM = pl.BlockSpec(memory_space=pltpu.SMEM)
HB = pl.BlockSpec(memory_space=pltpu.HBM)


def in_pairs(near, far, axis):
    size = lax.axis_size(axis)
    odd = [(i, ((i + 1) ^ 1) - 1) for i in range(1, size - 1)]
    got = lax.ppermute(far, axis, odd)
    return lax.ppermute(near, axis, [(i, i ^ 1) for i in range(size)]), got


def total(sums):
    size = sums.shape[0]
    sent = lax.all_to_all(sums.reshape(size, 1, LANES), ALL, 0, 0, tiled=True)
    return sent.reshape(size, LANES)


def body(phase, tile_mask):
    n, width = phase.shape
    f32 = jnp.float32
    sd = jax.ShapeDtypeStruct
    odd = jnp.stack([lax.axis_index(ROW) % 2, lax.axis_index(COL) % 2]).astype(jnp.int32)
    edge = sd((8, width + LANES), f32)
    near, far, own_mask = pl.pallas_call(
        strips_kernel,
        in_specs=[SM, HB, HB],
        out_specs=[VM] * 3,
        out_shape=[sd((8, n + LANES), f32)] * 2 + [sd((8, LANES), f32)],
        scratch_shapes=[
            pltpu.VMEM((n, LANES), f32),
            pltpu.VMEM((n, LANES), f32),
            pltpu.SMEM(tile_mask.shape, jnp.int32),
            pltpu.SemaphoreType.DMA((3,)),
        ],
        compiler_params=params(4),
        name="strips",
    )(odd, pltpu.with_memory_space_constraint(phase, pltpu.HBM), pltpu.with_memory_space_constraint(tile_mask, pltpu.HBM))
    near, far = in_pairs(near, far, COL)
    side, near, far, masks = pl.pallas_call(
        corners_kernel,
        in_specs=[SM] + [VM] * 4,
        out_specs=[VM] * 4,
        out_shape=[sd((n, LANES), f32), edge, edge, sd((2, 8, LANES), f32)],
        compiler_params=params(6),
        name="corners",
    )(odd, near, far, phase, own_mask)
    near, far = in_pairs(near, far, ROW)
    devices = 1
    for axis in ALL:
        devices *= lax.axis_size(axis)
    tiles = width // LANES + 1
    ext = sd((tiles, n + 32, LANES), f32)
    act = sd((tiles, 8 * (n // TILE + 2), LANES), f32)
    sums = sd((devices, LANES), f32)
    fields = [ext] * 5 + [act]
    *held, part = pl.pallas_call(
        inner_kernel,
        in_specs=[VM] * 4,
        out_specs=[VM] * 7,
        out_shape=fields + [sd((8, LANES), f32)],
        compiler_params=params(14),
        name="inner",
    )(phase, side, masks, own_mask)
    *held, part = pl.pallas_call(
        outer_kernel,
        in_specs=[SM] + [VM] * 9,
        out_specs=[VM] * 7,
        out_shape=fields + [sums],
        input_output_aliases={4 + i: i for i in range(6)},
        compiler_params=params(14),
        name="outer",
    )(odd, near, far, part, *held)
    p, w0, w1, w2, coef, act = held
    gathered = total(part)
    own = sd((n, width), f32)
    section, base, v0, v1, v2, part = pl.pallas_call(
        second_kernel,
        in_specs=[VM] * 7,
        out_specs=[HB] + [VM] * 5,
        out_shape=[own, own, ext, ext, ext, sums],
        scratch_shapes=[pltpu.VMEM((n, width), f32), pltpu.SemaphoreType.DMA(())],
        compiler_params=params(20),
        name="second",
    )(gathered, p, w0, w1, w2, coef, act)
    updated = pl.pallas_call(
        third_kernel,
        in_specs=[VM] * 5,
        out_specs=HB,
        out_shape=own,
        scratch_shapes=[pltpu.VMEM((n, width), f32), pltpu.SemaphoreType.DMA((CHUNKS,))],
        compiler_params=params(10),
        name="third",
    )(total(part), base, v0, v1, v2)
    return updated, section


def solution(mesh):
    split = Mesh(mesh.devices.reshape(4, 4, 4, 2), ALL)
    in_specs = (P(ROW, COL), P(ROW, COL))
    out_specs = (P(ROW, COL), P(ROW, COL))
    return jax.shard_map(body, mesh=split, in_specs=in_specs, out_specs=out_specs, check_vma=False)
```

```python
import jax
import jax.numpy as jnp
from jax import lax
from jax.experimental import pallas as pl
from jax.experimental.pallas import tpu as pltpu
from jax.sharding import Mesh
from jax.sharding import PartitionSpec as P


TILE = 256
ROW = ("row_0", "row_1")
COL = ("col_0", "col_1")
ALL = ROW + COL
LANES = 128
UNROLL = 33
CHUNKS = 4


def splat(row, lane, k):
    return jnp.broadcast_to(
        jnp.sum(jnp.where(lane == k, row, 0.0), axis=1, keepdims=True), (8, LANES)
    )


def matmul3(a, b):
    return [
        [a[i][0] * b[0][j] + a[i][1] * b[1][j] + a[i][2] * b[2][j] for j in range(3)]
        for i in range(3)
    ]


def phi_column(hess, scale, order):
    inv = 1.0 / 1024.0
    base = [[hess[i][j] * (scale * inv) for j in range(3)] for i in range(3)]
    zero = jnp.zeros((8, LANES), jnp.float32)
    term = base
    cols = [[zero + inv, zero, zero]] + [[zero] * 3 for _ in range(order - 1)]
    total = base
    sums = cols
    for degree in range(2, 11):
        first = [term[i][0] * (inv / degree) for i in range(3)]
        cols = [first] + [[c * (inv / degree) for c in col] for col in cols[:-1]]
        term = [[v * (1.0 / degree) for v in row] for row in matmul3(term, base)]
        total = [[total[i][j] + term[i][j] for j in range(3)] for i in range(3)]
        sums = [[s + c for s, c in zip(sc, cc)] for sc, cc in zip(sums, cols)]
    one, two = inv, 0.5 * inv * inv
    for _ in range(10):
        moved = []
        for n, col in enumerate(sums):
            new = [
                2.0 * col[i]
                + (total[i][0] * col[0] + total[i][1] * col[1] + total[i][2] * col[2])
                for i in range(3)
            ]
            if n >= 1:
                new = [new[i] + sums[n - 1][i] * one for i in range(3)]
            if n >= 2:
                new = [new[i] + sums[n - 2][i] * two for i in range(3)]
            moved.append(new)
        square = matmul3(total, total)
        total = [[2.0 * total[i][j] + square[i][j] for j in range(3)] for i in range(3)]
        sums = moved
        one, two = 2.0 * one, 2.0 * two + one * one
    return sums[-1]


def root(x):
    inv = lax.rsqrt(x)
    inv = inv * (1.5 - 0.5 * (x * inv) * inv)
    return x * inv, inv


def hessenberg(gathered):
    lane = lax.broadcasted_iota(jnp.int32, (8, LANES), 1)
    row = jnp.broadcast_to(jnp.sum(gathered, axis=0, keepdims=True), (8, LANES))
    m = [splat(row, lane, n) for n in range(6)]
    r00, i0 = root(m[0])
    r01, r02, r03 = m[1] * i0, m[2] * i0, m[3] * i0
    r11, i1 = root(jnp.maximum(m[2] - r01 * r01, 1e-9 * m[2]))
    r12, r13 = (m[3] - r01 * r02) * i1, (m[4] - r01 * r03) * i1
    r22, i2 = root(jnp.maximum(m[4] - r02 * r02 - r12 * r12, 1e-9 * m[4]))
    r23 = (m[5] - r02 * r03 - r12 * r13) * i2
    zero = jnp.zeros((8, LANES), jnp.float32)
    j0, j1, j2 = 8.0 * i0, 8.0 * i1, 8.0 * i2
    c0 = [r01 * j0, r11 * j0, zero]
    d0, d1 = 0.125 * c0[0], 0.125 * c0[1]
    c1 = [(r02 - d0 * r01) * j1, (r12 - d1 * r01) * j1, r22 * j1]
    e0, e1, e2 = [0.125 * v for v in c1]
    c2 = [(r03 - d0 * r02 - e0 * r12) * j2, (r13 - d1 * r02 - e1 * r12) * j2, (r23 - e2 * r12) * j2]
    hess = [[c0[i], c1[i], c2[i]] for i in range(3)]
    for i in range(3):
        hess[i][i] = hess[i][i] - 8.0
    return (r00, r01, r02, r12, i0, i1, i2), hess


def on_basis(r, weights, factor):
    r00, r01, r02, r12, i0, i1, i2 = r
    scale = factor * r00
    d2 = weights[2] * i2
    d1 = (weights[1] - r12 * d2) * i1
    d0 = (weights[0] - r01 * d1 - r02 * d2) * i0
    return [d0 * scale, d1 * scale, d2 * scale]


def beside(ref, at, sides):
    tiles = ref.shape[0]
    lane = lax.broadcasted_iota(jnp.int32, (8, LANES), 1)
    mids = [ref[j, pl.ds(at, 8), :] for j in range(tiles)]
    ones = [pltpu.roll(m, 1, 1) for m in mids]
    out = [jnp.where(lane == 0, ones[j - 1], ones[j]) for j in range(tiles)]
    if sides == 2:
        backs = [pltpu.roll(m, LANES - 1, 1) for m in mids]
        out = [o + jnp.where(lane == LANES - 1, backs[(j + 1) % tiles], backs[j]) for j, o in enumerate(out)]
    return out


def sum_row(sums):
    sub = lax.broadcasted_iota(jnp.int32, (8, LANES), 0)
    lane = lax.broadcasted_iota(jnp.int32, (8, LANES), 1)
    rows = jnp.zeros((8, LANES), jnp.float32)
    for n, tiles in enumerate(sums):
        part = jnp.sum(sum(tiles[1:], tiles[0]), axis=0, keepdims=True)
        rows = jnp.where(sub == n, part, rows)
    values = jnp.sum(rows, axis=1, keepdims=True)
    row = jnp.sum(jnp.where(lane == sub, values, 0.0), axis=0, keepdims=True)
    return jnp.broadcast_to(row, (8, LANES))


def write_row(row, out_ref):
    for i in range(0, out_ref.shape[0], 8):
        out_ref[i : i + 8, :] = row


def band_of(group, bands):
    return jnp.clip((group - 1 + TILE // 8) // (TILE // 8), 0, bands - 1)


def act_of(act_ref, group):
    bands = act_ref.shape[1] // 8
    if isinstance(group, int):
        band = 8 * min(max((group - 1 + TILE // 8) // (TILE // 8), 0), bands - 1)
    else:
        band = pl.multiple_of(8 * band_of(group, bands), 8)
    return [act_ref[j, pl.ds(band, 8), :] for j in range(act_ref.shape[0])]


def over_groups(lo, hi, emit, carry, most=UNROLL):
    unroll = min(most, hi - lo)
    while (hi - lo) % unroll:
        unroll -= 1

    def step(i, c):
        group = lo + i * unroll
        at = pl.multiple_of(8 + 8 * group, 8)
        for u in range(unroll):
            c = emit(group + u, at + 8 * u, c)
        return c

    if hi - lo == unroll:
        for g in range(lo, hi):
            carry = emit(g, 8 + 8 * g, carry)
        return carry
    return lax.fori_loop(0, (hi - lo) // unroll, step, carry)


def is_own(group, groups):
    return not isinstance(group, int) or 0 < group < groups - 1


def add_products(sums, pairs):
    return tuple(
        tuple(s + a[j] * b[j] for j, s in enumerate(row)) for row, (a, b) in zip(sums, pairs)
    )


def no_sums(count, tiles):
    return tuple(tuple(jnp.zeros((8, LANES), jnp.float32) for _ in range(tiles - 1)) for _ in range(count))


def power_of(src, dst, coef_ref, act_ref):
    tiles, rows, _ = src.shape
    groups = (rows - 16) // 8

    def emit(group, at, sums):
        side = beside(src, at, 2)
        acts = act_of(act_ref, group)
        here = pl.ds(at, 8)
        mids, outs = [], []
        for j in range(tiles):
            mid = src[j, here, :]
            total = side[j] + (src[j, pl.ds(at - 1, 8), :] + src[j, pl.ds(at + 1, 8), :])
            out = acts[j] * total + coef_ref[j, here, :] * mid
            dst[j, here, :] = out
            mids.append(mid)
            outs.append(out)
        return add_products(sums, ((mids, outs), (outs, outs))) if is_own(group, groups) else sums

    return emit


def form_of(src, coef_ref):
    tiles = src.shape[0]

    def emit(group, at, sums):
        side = beside(src, at, 1)
        here = pl.ds(at, 8)
        mids, images = [], []
        for j in range(tiles - 1):
            mid = src[j, here, :]
            images.append(0.5 * (side[j] + src[j, pl.ds(at - 1, 8), :]) + coef_ref[j, here, :] * mid)
            mids.append(mid)
        return add_products(sums, ((mids, images),))

    return emit


def force_of(p_ref, w0, coef_ref, act_ref):
    tiles, rows, _ = p_ref.shape
    groups = (rows - 16) // 8

    def emit(group, at, sums):
        side = beside(p_ref, at, 2)
        acts = act_of(act_ref, group)
        here = pl.ds(at, 8)
        outs = []
        for j in range(tiles):
            mid = p_ref[j, here, :]
            total = side[j] + (p_ref[j, pl.ds(at - 1, 8), :] + p_ref[j, pl.ds(at + 1, 8), :])
            square = mid * mid
            out = acts[j] * (8.0 * total - (28.0 + 4.0 * square) * mid)
            w0[j, here, :] = out
            coef_ref[j, here, :] = acts[j] * (0.5 - 1.5 * square)
            outs.append(out)
        return add_products(sums, ((outs, outs),)) if is_own(group, groups) else sums

    return emit


def strips_kernel(odd_ref, phase_hbm, mask_hbm, near_ref, far_ref, own_ref, left_ref, right_ref, mask_ref, sems):
    n, width = phase_hbm.shape
    copies = [
        pltpu.make_async_copy(phase_hbm.at[:, 0:LANES], left_ref, sems.at[0]),
        pltpu.make_async_copy(phase_hbm.at[:, width - LANES : width], right_ref, sems.at[1]),
        pltpu.make_async_copy(mask_hbm, mask_ref, sems.at[2]),
    ]
    for c in copies:
        c.start()
    for c in copies:
        c.wait()
    odd = jnp.full((8, LANES), odd_ref[1], jnp.int32) > 0
    odd_n = jnp.full((8, n), odd_ref[1], jnp.int32) > 0
    lane = lax.broadcasted_iota(jnp.int32, (8, LANES), 1)
    strips = []
    for ref, rows, col in ((left_ref, 0, 0), (right_ref, LANES - 8, mask_ref.shape[1] - 1)):
        extra = jnp.zeros((8, LANES), jnp.float32)
        for t in range(mask_ref.shape[0]):
            extra = extra + jnp.where(lane == t, mask_ref[t, col].astype(jnp.float32), 0.0)
        strips.append((ref[...].T[rows : rows + 8, :], extra))
    own = jnp.zeros((8, LANES), jnp.float32)
    tiles_r, tiles_c = mask_ref.shape
    for t in range(tiles_r):
        for c in range(tiles_c):
            own = jnp.where(lane == t * tiles_c + c, mask_ref[t, c].astype(jnp.float32), own)
    own_ref[...] = own
    left, right = strips
    for out, a, b in ((near_ref, left, right), (far_ref, right, left)):
        out[:, :n] = jnp.where(odd_n, a[0], b[0])
        out[:, n:] = jnp.where(odd, a[1], b[1])


def corners_kernel(odd_ref, near_in, far_in, phase_ref, own_ref, side_ref, near_ref, far_ref, masks_ref):
    n, width = phase_ref.shape
    tiles_r, tiles_c = n // TILE, width // TILE
    odd = jnp.full((8, LANES), odd_ref[1], jnp.int32) > 0
    odd_n = jnp.full((8, n), odd_ref[1], jnp.int32) > 0
    from_left = jnp.where(odd_n, near_in[:, :n], far_in[:, :n])
    from_right = jnp.where(odd_n, far_in[:, :n], near_in[:, :n])
    mask_left = jnp.where(odd, near_in[:, n:], far_in[:, n:])
    mask_right = jnp.where(odd, far_in[:, n:], near_in[:, n:])
    masks_ref[0] = mask_left
    masks_ref[1] = mask_right
    zeros = jnp.zeros((LANES - 16, n), jnp.float32)
    side = jnp.concatenate([from_right, zeros, from_left], axis=0).T
    side_ref[...] = side
    lane = lax.broadcasted_iota(jnp.int32, (8, LANES), 1)
    strips = []
    for rows, t in ((0, 0), (n - 8, tiles_r - 1)):
        extra = side[rows : rows + 8, :]
        for c in range(tiles_c):
            extra = jnp.where(lane == 16 + c, splat(own_ref[...], lane, t * tiles_c + c), extra)
        extra = jnp.where(lane == 16 + tiles_c, splat(mask_right, lane, t), extra)
        extra = jnp.where(lane == 17 + tiles_c, splat(mask_left, lane, t), extra)
        strips.append((phase_ref[rows : rows + 8, :], extra))
    up, down = strips
    odd = jnp.full((8, LANES), odd_ref[0], jnp.int32) > 0
    odd_w = jnp.full((8, width), odd_ref[0], jnp.int32) > 0
    for out, a, b in ((near_ref, up, down), (far_ref, down, up)):
        out[:, :width] = jnp.where(odd_w, a[0], b[0])
        out[:, width:] = jnp.where(odd, a[1], b[1])


def act_cells(act_ref, band, values, right, left):
    tiles = act_ref.shape[0]
    lane = lax.broadcasted_iota(jnp.int32, (8, LANES), 1)
    for j in range(tiles - 1):
        act_ref[j, 8 * band : 8 * band + 8, :] = 0.25 * values[j * LANES // TILE]
    ends = jnp.where(lane < 8, right, jnp.where(lane >= LANES - 8, left, 0.0))
    act_ref[tiles - 1, 8 * band : 8 * band + 8, :] = 0.25 * ends


def first_passes(p_ref, w0, w1, w2, coef_ref, act_ref):
    return (
        (force_of(p_ref, w0, coef_ref, act_ref), 1),
        (power_of(w0, w1, coef_ref, act_ref), 2),
        (power_of(w1, w2, coef_ref, act_ref), 2),
        (form_of(w2, coef_ref), 1),
    )


def inner_kernel(phase_ref, side_in, masks_ref, own_ref, p_ref, w0, w1, w2, coef_ref, act_ref, sums_ref):
    n, width = phase_ref.shape
    tiles = p_ref.shape[0]
    groups = n // 8 + 2
    tiles_r, tiles_c = n // TILE, width // TILE
    lane = lax.broadcasted_iota(jnp.int32, (8, LANES), 1)
    for t in range(tiles_r):
        values = [splat(own_ref[...], lane, t * tiles_c + c) for c in range(tiles_c)]
        act_cells(act_ref, t + 1, values, splat(masks_ref[1], lane, t), splat(masks_ref[0], lane, t))
    for j in range(tiles - 1):
        p_ref[j, 16 : n + 16, :] = phase_ref[:, j * LANES : (j + 1) * LANES]
    p_ref[tiles - 1, 16 : n + 16, :] = side_in[...]
    sums = []
    for k, (emit, count) in enumerate(first_passes(p_ref, w0, w1, w2, coef_ref, act_ref)):
        sums += over_groups(2 + k, groups - 2 - k, emit, no_sums(count, tiles))
    sums_ref[...] = sum_row(sums)


def outer_kernel(
    odd_ref, near_in, far_in, inner_ref, p_in, w0_in, w1_in, w2_in, coef_in, act_in,
    p_ref, w0, w1, w2, coef_ref, act_ref, sums_ref,
):
    tiles, rows, _ = p_ref.shape
    n = rows - 32
    groups = n // 8 + 2
    width = LANES * (tiles - 1)
    tiles_r, tiles_c = n // TILE, width // TILE
    lane = lax.broadcasted_iota(jnp.int32, (8, LANES), 1)
    odd = jnp.full((8, LANES), odd_ref[0], jnp.int32) > 0
    up = [jnp.where(odd, near_in[:, j * LANES : (j + 1) * LANES], far_in[:, j * LANES : (j + 1) * LANES]) for j in range(tiles)]
    down = [jnp.where(odd, far_in[:, j * LANES : (j + 1) * LANES], near_in[:, j * LANES : (j + 1) * LANES]) for j in range(tiles)]
    for t, extra in ((0, up[-1]), (tiles_r + 1, down[-1])):
        values = [splat(extra, lane, 16 + c) for c in range(tiles_c + 2)]
        act_cells(act_ref, t, values[:tiles_c], values[tiles_c], values[tiles_c + 1])
    blank = jnp.zeros((8, LANES), jnp.float32)
    for ref in (p_ref, w0, w1, w2):
        for j in range(tiles):
            ref[j, 0:8, :] = blank
            ref[j, n + 24 : n + 32, :] = blank
    for at, strip in ((8, up), (n + 16, down)):
        for j in range(tiles - 1):
            p_ref[j, at : at + 8, :] = strip[j]
        p_ref[tiles - 1, at : at + 8, :] = jnp.where((lane < 8) | (lane >= LANES - 8), strip[-1], 0.0)
    sums = []
    for k, (emit, count) in enumerate(first_passes(p_ref, w0, w1, w2, coef_ref, act_ref)):
        own = k == 3
        part = no_sums(count, tiles)
        part = over_groups(1 if own else 0, 2 + k, emit, part)
        sums += over_groups(groups - 2 - k, groups - 1 if own else groups, emit, part)
    write_row(sum_row(sums) + inner_ref[...], sums_ref)


def second_kernel(
    gathered_ref, p_ref, w0, w1, w2, coef_ref, act_ref,
    section_hbm, base_ref, v0, v1, v2, sums_ref, section_ref, sem,
):
    tiles, rows, _ = p_ref.shape
    groups = (rows - 16) // 8
    r, hess = hessenberg(gathered_ref[...])
    scale = jnp.where(lax.broadcasted_iota(jnp.int32, (8, LANES), 0) < 4, 0.5, 1.0)
    coefs = on_basis(r, phi_column(hess, scale, 1), scale)
    a = [jnp.broadcast_to(c[0:1], (8, LANES)) for c in coefs]
    f = [jnp.broadcast_to(c[7:8], (8, LANES)) for c in coefs]
    blank = jnp.zeros((8, LANES), jnp.float32)
    for ref in (v0, v1, v2):
        for j in range(tiles):
            ref[j, 0:8, :] = blank
            ref[j, rows - 8 : rows, :] = blank

    def start(group, at, sums):
        acts = act_of(act_ref, group)
        here = pl.ds(at, 8)
        own = is_own(group, groups)
        outs = []
        for j in range(tiles):
            ws = [ref[j, here, :] for ref in (w0, w1, w2)]
            phase = p_ref[j, here, :]
            shift = a[0] * ws[0] + a[1] * ws[1] + a[2] * ws[2]
            out = (acts[j] * (shift * shift)) * (shift + 3.0 * phase)
            v0[j, here, :] = out
            outs.append(out)
            if own and j < tiles - 1:
                to = pl.ds(pl.multiple_of(at - 16, 8), 8)
                cols = slice(j * LANES, (j + 1) * LANES)
                section_ref[to, cols] = phase + shift
                base_ref[to, cols] = phase + (f[0] * ws[0] + f[1] * ws[1] + f[2] * ws[2])
        return add_products(sums, ((outs, outs),)) if own else sums

    def sides(emit, count, most):
        part = over_groups(0, 1, emit, no_sums(count, tiles))
        part = over_groups(1, groups - 1, emit, part, most)
        return over_groups(groups - 1, groups, emit, part)

    sums = [*sides(start, 1, 8)]
    copy = pltpu.make_async_copy(section_ref, section_hbm, sem)
    copy.start()
    sums += sides(power_of(v0, v1, coef_ref, act_ref), 2, UNROLL)
    sums += sides(power_of(v1, v2, coef_ref, act_ref), 2, UNROLL)
    sums += over_groups(1, groups - 1, form_of(v2, coef_ref), no_sums(1, tiles))
    write_row(sum_row(sums), sums_ref)
    copy.wait()


def third_kernel(gathered_ref, base_ref, v0, v1, v2, updated_hbm, updated_ref, sems):
    n, width = base_ref.shape
    r, hess = hessenberg(gathered_ref[...])
    d = on_basis(r, phi_column(hess, 1.0, 3), -4.0 * 32.0)

    def emit(group, at, c):
        here = pl.ds(at, 8)
        to = pl.ds(pl.multiple_of(at - 16, 8), 8)
        for j in range(width // LANES):
            cols = slice(j * LANES, (j + 1) * LANES)
            updated_ref[to, cols] = base_ref[to, cols] + (
                d[0] * v0[j, here, :] + d[1] * v1[j, here, :] + d[2] * v2[j, here, :]
            )
        return c

    copies = []
    chunk = n // CHUNKS
    for k in range(CHUNKS):
        over_groups(1 + k * chunk // 8, 1 + (k + 1) * chunk // 8, emit, 0, 4)
        part = pl.ds(k * chunk, chunk)
        copies.append(pltpu.make_async_copy(updated_ref.at[part, :], updated_hbm.at[part, :], sems.at[k]))
        copies[-1].start()
    for copy in copies:
        copy.wait()


def params(mib):
    return pltpu.CompilerParams(vmem_limit_bytes=mib << 20)


VM = pl.BlockSpec(memory_space=pltpu.VMEM)
SM = pl.BlockSpec(memory_space=pltpu.SMEM)
HB = pl.BlockSpec(memory_space=pltpu.HBM)


def in_pairs(near, far, axis):
    size = lax.axis_size(axis)
    odd = [(i, ((i + 1) ^ 1) - 1) for i in range(1, size - 1)]
    far = lax.ppermute(far, axis, odd)
    near = lax.ppermute(near, axis, [(i, i ^ 1) for i in range(size)])
    return near, far


def total(sums):
    size = sums.shape[0]
    sent = lax.all_to_all(sums.reshape(size, 1, LANES), ALL[::-1], 0, 0, tiled=True)
    return sent.reshape(size, LANES)


def step(phase, tile_mask):
    n, width = phase.shape
    f32 = jnp.float32
    sd = jax.ShapeDtypeStruct
    odd = jnp.stack([lax.axis_index(ROW) % 2, lax.axis_index(COL) % 2]).astype(jnp.int32)
    edge = sd((8, width + LANES), f32)
    near, far, own_mask = pl.pallas_call(
        strips_kernel,
        in_specs=[SM, HB, HB],
        out_specs=[VM] * 3,
        out_shape=[sd((8, n + LANES), f32)] * 2 + [sd((8, LANES), f32)],
        scratch_shapes=[
            pltpu.VMEM((n, LANES), f32),
            pltpu.VMEM((n, LANES), f32),
            pltpu.SMEM(tile_mask.shape, jnp.int32),
            pltpu.SemaphoreType.DMA((3,)),
        ],
        compiler_params=params(4),
        name="strips",
    )(odd, pltpu.with_memory_space_constraint(phase, pltpu.HBM), pltpu.with_memory_space_constraint(tile_mask, pltpu.HBM))
    near, far = in_pairs(near, far, COL)
    side, near, far, masks = pl.pallas_call(
        corners_kernel,
        in_specs=[SM] + [VM] * 4,
        out_specs=[VM] * 4,
        out_shape=[sd((n, LANES), f32), edge, edge, sd((2, 8, LANES), f32)],
        compiler_params=params(6),
        name="corners",
    )(odd, near, far, phase, own_mask)
    near, far = in_pairs(near, far, ROW)
    devices = 1
    for axis in ALL:
        devices *= lax.axis_size(axis)
    tiles = width // LANES + 1
    ext = sd((tiles, n + 32, LANES), f32)
    act = sd((tiles, 8 * (n // TILE + 2), LANES), f32)
    sums = sd((devices, LANES), f32)
    fields = [ext] * 5 + [act]
    *held, part = pl.pallas_call(
        inner_kernel,
        in_specs=[VM] * 4,
        out_specs=[VM] * 7,
        out_shape=fields + [sd((8, LANES), f32)],
        compiler_params=params(14),
        name="inner",
    )(phase, side, masks, own_mask)
    *held, part = pl.pallas_call(
        outer_kernel,
        in_specs=[SM] + [VM] * 9,
        out_specs=[VM] * 7,
        out_shape=fields + [sums],
        input_output_aliases={4 + i: i for i in range(6)},
        compiler_params=params(14),
        name="outer",
    )(odd, near, far, part, *held)
    p, w0, w1, w2, coef, act = held
    gathered = total(part)
    own = sd((n, width), f32)
    section, base, v0, v1, v2, part = pl.pallas_call(
        second_kernel,
        in_specs=[VM] * 7,
        out_specs=[HB] + [VM] * 5,
        out_shape=[own, own, ext, ext, ext, sums],
        scratch_shapes=[pltpu.VMEM((n, width), f32), pltpu.SemaphoreType.DMA(())],
        compiler_params=params(20),
        name="second",
    )(gathered, p, w0, w1, w2, coef, act)
    updated = pl.pallas_call(
        third_kernel,
        in_specs=[VM] * 5,
        out_specs=HB,
        out_shape=own,
        scratch_shapes=[pltpu.VMEM((n, width), f32), pltpu.SemaphoreType.DMA((CHUNKS,))],
        compiler_params=params(10),
        name="third",
    )(total(part), base, v0, v1, v2)
    return updated, section


def solution(mesh):
    split = Mesh(mesh.devices.reshape(4, 4, 4, 2), ALL)
    in_specs = (P(ROW, COL), P(ROW, COL))
    out_specs = (P(ROW, COL), P(ROW, COL))
    return jax.shard_map(step, mesh=split, in_specs=in_specs, out_specs=out_specs, check_vma=False)
```

```python
import functools

import jax
import jax.numpy as jnp
from jax import lax
from jax.experimental import pallas as pl
from jax.experimental.pallas import tpu as pltpu
from jax.sharding import Mesh
from jax.sharding import PartitionSpec as P


TILE = 256
ROW = ("row_0", "row_1")
COL = ("col_0", "col_1")
ALL = ROW + COL
LANES = 128
UNROLL = 33
CHUNKS = 4


def splat(row, lane, k):
    return jnp.broadcast_to(
        jnp.sum(jnp.where(lane == k, row, 0.0), axis=1, keepdims=True), (8, LANES)
    )


def matmul3(a, b):
    return [
        [a[i][0] * b[0][j] + a[i][1] * b[1][j] + a[i][2] * b[2][j] for j in range(3)]
        for i in range(3)
    ]


def phi_column(hess, scale, order):
    inv = 1.0 / 1024.0
    base = [[hess[i][j] * (scale * inv) for j in range(3)] for i in range(3)]
    zero = jnp.zeros((8, LANES), jnp.float32)
    term = base
    cols = [[zero + inv, zero, zero]] + [[zero] * 3 for _ in range(order - 1)]
    total = base
    sums = cols
    for degree in range(2, 11):
        first = [term[i][0] * (inv / degree) for i in range(3)]
        cols = [first] + [[c * (inv / degree) for c in col] for col in cols[:-1]]
        term = [[v * (1.0 / degree) for v in row] for row in matmul3(term, base)]
        total = [[total[i][j] + term[i][j] for j in range(3)] for i in range(3)]
        sums = [[s + c for s, c in zip(sc, cc)] for sc, cc in zip(sums, cols)]
    one, two = inv, 0.5 * inv * inv
    for _ in range(10):
        moved = []
        for n, col in enumerate(sums):
            new = [
                2.0 * col[i]
                + (total[i][0] * col[0] + total[i][1] * col[1] + total[i][2] * col[2])
                for i in range(3)
            ]
            if n >= 1:
                new = [new[i] + sums[n - 1][i] * one for i in range(3)]
            if n >= 2:
                new = [new[i] + sums[n - 2][i] * two for i in range(3)]
            moved.append(new)
        square = matmul3(total, total)
        total = [[2.0 * total[i][j] + square[i][j] for j in range(3)] for i in range(3)]
        sums = moved
        one, two = 2.0 * one, 2.0 * two + one * one
    return sums[-1]


def root(x):
    inv = lax.rsqrt(x)
    inv = inv * (1.5 - 0.5 * (x * inv) * inv)
    return x * inv, inv


def hessenberg(gathered):
    lane = lax.broadcasted_iota(jnp.int32, (8, LANES), 1)
    row = jnp.broadcast_to(jnp.sum(gathered, axis=0, keepdims=True), (8, LANES))
    m = [splat(row, lane, n) for n in range(6)]
    r00, i0 = root(m[0])
    r01, r02, r03 = m[1] * i0, m[2] * i0, m[3] * i0
    r11, i1 = root(jnp.maximum(m[2] - r01 * r01, 1e-9 * m[2]))
    r12, r13 = (m[3] - r01 * r02) * i1, (m[4] - r01 * r03) * i1
    r22, i2 = root(jnp.maximum(m[4] - r02 * r02 - r12 * r12, 1e-9 * m[4]))
    r23 = (m[5] - r02 * r03 - r12 * r13) * i2
    zero = jnp.zeros((8, LANES), jnp.float32)
    j0, j1, j2 = 8.0 * i0, 8.0 * i1, 8.0 * i2
    c0 = [r01 * j0, r11 * j0, zero]
    d0, d1 = 0.125 * c0[0], 0.125 * c0[1]
    c1 = [(r02 - d0 * r01) * j1, (r12 - d1 * r01) * j1, r22 * j1]
    e0, e1, e2 = [0.125 * v for v in c1]
    c2 = [(r03 - d0 * r02 - e0 * r12) * j2, (r13 - d1 * r02 - e1 * r12) * j2, (r23 - e2 * r12) * j2]
    hess = [[c0[i], c1[i], c2[i]] for i in range(3)]
    for i in range(3):
        hess[i][i] = hess[i][i] - 8.0
    return (r00, r01, r02, r12, i0, i1, i2), hess


def on_basis(r, weights, factor):
    r00, r01, r02, r12, i0, i1, i2 = r
    scale = factor * r00
    d2 = weights[2] * i2
    d1 = (weights[1] - r12 * d2) * i1
    d0 = (weights[0] - r01 * d1 - r02 * d2) * i0
    return [d0 * scale, d1 * scale, d2 * scale]


def beside(ref, at, sides):
    tiles = ref.shape[0]
    lane = lax.broadcasted_iota(jnp.int32, (8, LANES), 1)
    mids = [ref[j, pl.ds(at, 8), :] for j in range(tiles)]
    ones = [pltpu.roll(m, 1, 1) for m in mids]
    out = [jnp.where(lane == 0, ones[j - 1], ones[j]) for j in range(tiles)]
    if sides == 2:
        backs = [pltpu.roll(m, LANES - 1, 1) for m in mids]
        out = [o + jnp.where(lane == LANES - 1, backs[(j + 1) % tiles], backs[j]) for j, o in enumerate(out)]
    return out


def sum_row(sums):
    sub = lax.broadcasted_iota(jnp.int32, (8, LANES), 0)
    lane = lax.broadcasted_iota(jnp.int32, (8, LANES), 1)
    rows = jnp.zeros((8, LANES), jnp.float32)
    for n, tiles in enumerate(sums):
        part = jnp.sum(sum(tiles[1:], tiles[0]), axis=0, keepdims=True)
        rows = jnp.where(sub == n, part, rows)
    values = jnp.sum(rows, axis=1, keepdims=True)
    row = jnp.sum(jnp.where(lane == sub, values, 0.0), axis=0, keepdims=True)
    return jnp.broadcast_to(row, (8, LANES))


def write_row(row, out_ref):
    for i in range(0, out_ref.shape[0], 8):
        out_ref[i : i + 8, :] = row


def band_of(group, bands):
    return jnp.clip((group - 1 + TILE // 8) // (TILE // 8), 0, bands - 1)


def act_of(act_ref, group):
    bands = act_ref.shape[1] // 8
    if isinstance(group, int):
        band = 8 * min(max((group - 1 + TILE // 8) // (TILE // 8), 0), bands - 1)
    else:
        band = pl.multiple_of(8 * band_of(group, bands), 8)
    return [act_ref[j, pl.ds(band, 8), :] for j in range(act_ref.shape[0])]


def over_groups(lo, hi, emit, carry, most=UNROLL):
    unroll = min(most, hi - lo)
    while (hi - lo) % unroll:
        unroll -= 1

    def step(i, c):
        group = lo + i * unroll
        at = pl.multiple_of(8 + 8 * group, 8)
        for u in range(unroll):
            c = emit(group + u, at + 8 * u, c)
        return c

    if hi - lo == unroll:
        for g in range(lo, hi):
            carry = emit(g, 8 + 8 * g, carry)
        return carry
    return lax.fori_loop(0, (hi - lo) // unroll, step, carry)


def is_own(group, groups):
    return not isinstance(group, int) or 0 < group < groups - 1


def add_products(sums, pairs):
    return tuple(
        tuple(s + a[j] * b[j] for j, s in enumerate(row)) for row, (a, b) in zip(sums, pairs)
    )


def no_sums(count, tiles):
    return tuple(tuple(jnp.zeros((8, LANES), jnp.float32) for _ in range(tiles - 1)) for _ in range(count))


def power_of(src, dst, coef_ref, act_ref):
    tiles, rows, _ = src.shape
    groups = (rows - 16) // 8

    def emit(group, at, sums):
        side = beside(src, at, 2)
        acts = act_of(act_ref, group)
        here = pl.ds(at, 8)
        mids, outs = [], []
        for j in range(tiles):
            mid = src[j, here, :]
            total = side[j] + (src[j, pl.ds(at - 1, 8), :] + src[j, pl.ds(at + 1, 8), :])
            out = acts[j] * total + coef_ref[j, here, :] * mid
            dst[j, here, :] = out
            mids.append(mid)
            outs.append(out)
        return add_products(sums, ((mids, outs), (outs, outs))) if is_own(group, groups) else sums

    return emit


def form_of(src, coef_ref):
    tiles = src.shape[0]

    def emit(group, at, sums):
        side = beside(src, at, 1)
        here = pl.ds(at, 8)
        mids, images = [], []
        for j in range(tiles - 1):
            mid = src[j, here, :]
            images.append(0.5 * (side[j] + src[j, pl.ds(at - 1, 8), :]) + coef_ref[j, here, :] * mid)
            mids.append(mid)
        return add_products(sums, ((mids, images),))

    return emit


def force_of(p_ref, w0, coef_ref, act_ref):
    tiles, rows, _ = p_ref.shape
    groups = (rows - 16) // 8

    def emit(group, at, sums):
        side = beside(p_ref, at, 2)
        acts = act_of(act_ref, group)
        here = pl.ds(at, 8)
        outs = []
        for j in range(tiles):
            mid = p_ref[j, here, :]
            total = side[j] + (p_ref[j, pl.ds(at - 1, 8), :] + p_ref[j, pl.ds(at + 1, 8), :])
            square = mid * mid
            out = acts[j] * (8.0 * total - (28.0 + 4.0 * square) * mid)
            w0[j, here, :] = out
            coef_ref[j, here, :] = acts[j] * (0.5 - 1.5 * square)
            outs.append(out)
        return add_products(sums, ((outs, outs),)) if is_own(group, groups) else sums

    return emit


def rows_of(values):
    sub = lax.broadcasted_iota(jnp.int32, (8, LANES), 0)
    out = jnp.zeros((8, LANES), jnp.float32)
    for k, v in enumerate(values):
        out = jnp.where(sub == k, v, out)
    return out


def row_of(block, k):
    return jnp.broadcast_to(block[k : k + 1], (8, LANES))


def strips_kernel(odd_ref, phase_hbm, mask_hbm, near_ref, far_ref, own_ref, p_ref, mask_ref, sems):
    n, width = phase_hbm.shape
    last = width // LANES - 1
    copies = {}
    for j in (0, last, *range(1, last)):
        source = phase_hbm.at[:, j * LANES : (j + 1) * LANES]
        copies[j] = pltpu.make_async_copy(source, p_ref.at[j, 16 : n + 16, :], sems.at[j])
        copies[j].start()
    mask_copy = pltpu.make_async_copy(mask_hbm, mask_ref, sems.at[last + 1])
    mask_copy.start()
    mask_copy.wait()
    odd = jnp.full((8, LANES), odd_ref[1], jnp.int32) > 0
    odd_n = jnp.full((8, n), odd_ref[1], jnp.int32) > 0
    tiles_r, tiles_c = mask_ref.shape
    mask = [[mask_ref[t, c].astype(jnp.float32) for c in range(tiles_c)] for t in range(tiles_r)]
    own_ref[...] = rows_of([v for row in mask for v in row])
    copies[0].wait()
    copies[last].wait()
    strips = []
    for j, rows, col in ((0, 0, 0), (last, LANES - 8, -1)):
        strip = p_ref[j, 16 : n + 16, :].T[rows : rows + 8, :]
        strips.append((strip, rows_of([row[col] for row in mask])))
    left, right = strips
    for out, a, b in ((near_ref, left, right), (far_ref, right, left)):
        out[:, :n] = jnp.where(odd_n, a[0], b[0])
        out[:, n:] = jnp.where(odd, a[1], b[1])
    for j in range(1, last):
        copies[j].wait()


def corners_kernel(odd_ref, near_in, far_in, p_ref, own_ref, ends_ref, masks_ref, near_ref, far_ref):
    tiles, rows, _ = p_ref.shape
    n, width = rows - 32, LANES * (tiles - 1)
    tiles_r, tiles_c = n // TILE, width // TILE
    odd = jnp.full((8, LANES), odd_ref[1], jnp.int32) > 0
    odd_n = jnp.full((8, n), odd_ref[1], jnp.int32) > 0
    from_left = jnp.where(odd_n, near_in[:, :n], far_in[:, :n])
    from_right = jnp.where(odd_n, far_in[:, :n], near_in[:, :n])
    mask_left = jnp.where(odd, near_in[:, n:], far_in[:, n:])
    mask_right = jnp.where(odd, far_in[:, n:], near_in[:, n:])
    ends_ref[0] = from_right
    ends_ref[1] = from_left
    masks_ref[0] = mask_left
    masks_ref[1] = mask_right
    zeros = jnp.zeros((LANES - 16, LANES), jnp.float32)
    own = own_ref[...]
    odd_row = jnp.full((8, LANES), odd_ref[0], jnp.int32) > 0
    strips = []
    for at, part, row, t in ((16, slice(0, LANES), 0, 0), (n + 8, slice(n - LANES, n), LANES - 8, tiles_r - 1)):
        corner = jnp.concatenate([from_right[:, part], zeros, from_left[:, part]], axis=0).T[row : row + 8, :]
        masks = [row_of(own, t * tiles_c + c) for c in range(tiles_c)]
        masks += [row_of(mask_right, t), row_of(mask_left, t)]
        strips.append([p_ref[j, at : at + 8, :] for j in range(tiles - 1)] + [corner, rows_of(masks)])
    up, down = strips
    for out, a, b in ((near_ref, up, down), (far_ref, down, up)):
        for j in range(tiles + 1):
            out[:, j * LANES : (j + 1) * LANES] = jnp.where(odd_row, a[j], b[j])


def act_cells(act_ref, band, values, right, left):
    tiles = act_ref.shape[0]
    lane = lax.broadcasted_iota(jnp.int32, (8, LANES), 1)
    for j in range(tiles - 1):
        act_ref[j, 8 * band : 8 * band + 8, :] = 0.25 * values[j * LANES // TILE]
    ends = jnp.where(lane < 8, right, jnp.where(lane >= LANES - 8, left, 0.0))
    act_ref[tiles - 1, 8 * band : 8 * band + 8, :] = 0.25 * ends


def first_passes(p_ref, w0, w1, w2, coef_ref, act_ref):
    return (
        (force_of(p_ref, w0, coef_ref, act_ref), 1),
        (power_of(w0, w1, coef_ref, act_ref), 2),
        (power_of(w1, w2, coef_ref, act_ref), 2),
        (form_of(w2, coef_ref), 1),
    )


def inner_kernel(ends_ref, masks_ref, own_ref, p_in, p_ref, w0, w1, w2, coef_ref, act_ref, sums_ref):
    tiles, rows, _ = p_ref.shape
    n, width = rows - 32, LANES * (tiles - 1)
    groups = n // 8 + 2
    tiles_r, tiles_c = n // TILE, width // TILE
    for t in range(tiles_r):
        values = [row_of(own_ref[...], t * tiles_c + c) for c in range(tiles_c)]
        act_cells(act_ref, t + 1, values, row_of(masks_ref[1], t), row_of(masks_ref[0], t))
    zeros = jnp.zeros((LANES - 16, n), jnp.float32)
    p_ref[tiles - 1, 16 : n + 16, :] = jnp.concatenate([ends_ref[0], zeros, ends_ref[1]], axis=0).T
    sums = []
    for k, (emit, count) in enumerate(first_passes(p_ref, w0, w1, w2, coef_ref, act_ref)):
        sums += over_groups(2 + k, groups - 2 - k, emit, no_sums(count, tiles))
    sums_ref[...] = sum_row(sums)


def outer_kernel(
    odd_ref, near_in, far_in, inner_ref, p_in, w0_in, w1_in, w2_in, coef_in, act_in,
    p_ref, w0, w1, w2, coef_ref, act_ref, sums_ref,
):
    tiles, rows, _ = p_ref.shape
    n = rows - 32
    groups = n // 8 + 2
    width = LANES * (tiles - 1)
    tiles_r, tiles_c = n // TILE, width // TILE
    odd = jnp.full((8, LANES), odd_ref[0], jnp.int32) > 0
    near = [near_in[:, j * LANES : (j + 1) * LANES] for j in range(tiles + 1)]
    far = [far_in[:, j * LANES : (j + 1) * LANES] for j in range(tiles + 1)]
    *up, up_masks = [jnp.where(odd, a, b) for a, b in zip(near, far)]
    *down, down_masks = [jnp.where(odd, b, a) for a, b in zip(near, far)]
    for t, masks in ((0, up_masks), (tiles_r + 1, down_masks)):
        values = [row_of(masks, c) for c in range(tiles_c + 2)]
        act_cells(act_ref, t, values[:tiles_c], values[tiles_c], values[tiles_c + 1])
    blank = jnp.zeros((8, LANES), jnp.float32)
    for ref in (p_ref, w0, w1, w2):
        for j in range(tiles):
            ref[j, 0:8, :] = blank
            ref[j, n + 24 : n + 32, :] = blank
    for at, strip in ((8, up), (n + 16, down)):
        for j in range(tiles):
            p_ref[j, at : at + 8, :] = strip[j]
    sums = []
    for k, (emit, count) in enumerate(first_passes(p_ref, w0, w1, w2, coef_ref, act_ref)):
        own = k == 3
        part = no_sums(count, tiles)
        part = over_groups(1 if own else 0, 2 + k, emit, part)
        sums += over_groups(groups - 2 - k, groups - 1 if own else groups, emit, part)
    write_row(sum_row(sums) + inner_ref[...], sums_ref)


def second_kernel(
    gathered_ref, p_ref, w0, w1, w2, coef_ref, act_ref,
    section_hbm, base_ref, v0, v1, v2, sums_ref, section_ref, sem,
):
    tiles, rows, _ = p_ref.shape
    groups = (rows - 16) // 8
    r, hess = hessenberg(gathered_ref[...])
    scale = jnp.where(lax.broadcasted_iota(jnp.int32, (8, LANES), 0) < 4, 0.5, 1.0)
    coefs = on_basis(r, phi_column(hess, scale, 1), scale)
    a = [jnp.broadcast_to(c[0:1], (8, LANES)) for c in coefs]
    f = [jnp.broadcast_to(c[7:8], (8, LANES)) for c in coefs]
    blank = jnp.zeros((8, LANES), jnp.float32)
    for ref in (v0, v1, v2):
        for j in range(tiles):
            ref[j, 0:8, :] = blank
            ref[j, rows - 8 : rows, :] = blank

    def start(group, at, sums):
        acts = act_of(act_ref, group)
        here = pl.ds(at, 8)
        own = is_own(group, groups)
        outs = []
        for j in range(tiles):
            ws = [ref[j, here, :] for ref in (w0, w1, w2)]
            phase = p_ref[j, here, :]
            shift = a[0] * ws[0] + a[1] * ws[1] + a[2] * ws[2]
            out = (acts[j] * (shift * shift)) * (shift + 3.0 * phase)
            v0[j, here, :] = out
            outs.append(out)
            if own and j < tiles - 1:
                to = pl.ds(at - 16 if isinstance(at, int) else pl.multiple_of(at - 16, 8), 8)
                cols = slice(j * LANES, (j + 1) * LANES)
                section_ref[to, cols] = phase + shift
                base_ref[to, cols] = phase + (f[0] * ws[0] + f[1] * ws[1] + f[2] * ws[2])
        return add_products(sums, ((outs, outs),)) if own else sums

    def sides(emit, count, most):
        part = over_groups(0, 1, emit, no_sums(count, tiles))
        part = over_groups(1, groups - 1, emit, part, most)
        return over_groups(groups - 1, groups, emit, part)

    power = power_of(v0, v1, coef_ref, act_ref)

    def fused(group, at, c):
        return start(group, at, c[0]), power(group - 2, at - 16, c[1])

    part = no_sums(1, tiles), no_sums(2, tiles)
    part = over_groups(0, 3, start, part[0]), over_groups(0, 1, power, part[1])
    part = over_groups(3, groups - 1, fused, part)
    part = over_groups(groups - 1, groups, start, part[0]), part[1]
    copy = pltpu.make_async_copy(section_ref, section_hbm, sem)
    copy.start()
    sums = [*part[0], *over_groups(groups - 3, groups, power, part[1])]
    sums += sides(power_of(v1, v2, coef_ref, act_ref), 2, UNROLL)
    sums += over_groups(1, groups - 1, form_of(v2, coef_ref), no_sums(1, tiles))
    write_row(sum_row(sums), sums_ref)
    copy.wait()


def third_kernel(gathered_ref, base_ref, v0, v1, v2, updated_hbm, updated_ref, sems):
    n, width = base_ref.shape
    r, hess = hessenberg(gathered_ref[...])
    d = on_basis(r, phi_column(hess, 1.0, 3), -4.0 * 32.0)

    def emit(group, at, c):
        here = pl.ds(at, 8)
        to = pl.ds(pl.multiple_of(at - 16, 8), 8)
        for j in range(width // LANES):
            cols = slice(j * LANES, (j + 1) * LANES)
            updated_ref[to, cols] = base_ref[to, cols] + (
                d[0] * v0[j, here, :] + d[1] * v1[j, here, :] + d[2] * v2[j, here, :]
            )
        return c

    copies = []
    chunk = n // CHUNKS
    for k in range(CHUNKS):
        over_groups(1 + k * chunk // 8, 1 + (k + 1) * chunk // 8, emit, 0, 4)
        part = pl.ds(k * chunk, chunk)
        copies.append(pltpu.make_async_copy(updated_ref.at[part, :], updated_hbm.at[part, :], sems.at[k]))
        copies[-1].start()
    for copy in copies:
        copy.wait()


def params(mib):
    return pltpu.CompilerParams(vmem_limit_bytes=mib << 20)


VM = pl.BlockSpec(memory_space=pltpu.VMEM)
SM = pl.BlockSpec(memory_space=pltpu.SMEM)
HB = pl.BlockSpec(memory_space=pltpu.HBM)


def in_pairs(near, far, axis):
    size = lax.axis_size(axis)
    odd = [(i, ((i + 1) ^ 1) - 1) for i in range(1, size - 1)]
    far = lax.ppermute(far, axis, odd)
    near = lax.ppermute(near, axis, [(i, i ^ 1) for i in range(size)])
    return near, far


def total(sums):
    size = sums.shape[0]
    sent = lax.all_to_all(sums.reshape(size, 1, LANES), ALL[::-1], 0, 0, tiled=True)
    return sent.reshape(size, LANES)


def step(phase, tile_mask):
    n, width = phase.shape
    f32 = jnp.float32
    sd = jax.ShapeDtypeStruct
    odd = jnp.stack([lax.axis_index(ROW) % 2, lax.axis_index(COL) % 2]).astype(jnp.int32)
    tiles = width // LANES + 1
    ext = sd((tiles, n + 32, LANES), f32)
    act = sd((tiles, 8 * (n // TILE + 2), LANES), f32)
    edge = sd((8, width + 2 * LANES), f32)
    hbm = functools.partial(pltpu.with_memory_space_constraint, memory_space=pltpu.HBM)
    near, far, own_mask, p = pl.pallas_call(
        strips_kernel,
        in_specs=[SM, HB, HB],
        out_specs=[VM] * 4,
        out_shape=[sd((8, n + LANES), f32)] * 2 + [sd((8, LANES), f32), ext],
        scratch_shapes=[pltpu.SMEM(tile_mask.shape, jnp.int32), pltpu.SemaphoreType.DMA((tiles,))],
        compiler_params=params(6),
        name="strips",
    )(odd, hbm(phase), hbm(tile_mask))
    near, far = in_pairs(near, far, COL)
    ends, masks, near, far = pl.pallas_call(
        corners_kernel,
        in_specs=[SM] + [VM] * 4,
        out_specs=[VM] * 4,
        out_shape=[sd((2, 8, n), f32), sd((2, 8, LANES), f32), edge, edge],
        compiler_params=params(6),
        name="corners",
    )(odd, near, far, p, own_mask)
    near, far = in_pairs(near, far, ROW)
    devices = 1
    for axis in ALL:
        devices *= lax.axis_size(axis)
    sums = sd((devices, LANES), f32)
    fields = [ext] * 5 + [act]
    *held, part = pl.pallas_call(
        inner_kernel,
        in_specs=[VM] * 4,
        out_specs=[VM] * 7,
        out_shape=fields + [sd((8, LANES), f32)],
        input_output_aliases={3: 0},
        compiler_params=params(14),
        name="inner",
    )(ends, masks, own_mask, p)
    *held, part = pl.pallas_call(
        outer_kernel,
        in_specs=[SM] + [VM] * 9,
        out_specs=[VM] * 7,
        out_shape=fields + [sums],
        input_output_aliases={4 + i: i for i in range(6)},
        compiler_params=params(14),
        name="outer",
    )(odd, near, far, part, *held)
    p, w0, w1, w2, coef, act = held
    gathered = total(part)
    own = sd((n, width), f32)
    section, base, v0, v1, v2, part = pl.pallas_call(
        second_kernel,
        in_specs=[VM] * 7,
        out_specs=[HB] + [VM] * 5,
        out_shape=[own, own, ext, ext, ext, sums],
        scratch_shapes=[pltpu.VMEM((n, width), f32), pltpu.SemaphoreType.DMA(())],
        compiler_params=params(20),
        name="second",
    )(gathered, p, w0, w1, w2, coef, act)
    updated = pl.pallas_call(
        third_kernel,
        in_specs=[VM] * 5,
        out_specs=HB,
        out_shape=own,
        scratch_shapes=[pltpu.VMEM((n, width), f32), pltpu.SemaphoreType.DMA((CHUNKS,))],
        compiler_params=params(10),
        name="third",
    )(total(part), base, v0, v1, v2)
    return updated, section


def solution(mesh):
    split = Mesh(mesh.devices.reshape(4, 4, 4, 2), ALL)
    in_specs = (P(ROW, COL), P(ROW, COL))
    out_specs = (P(ROW, COL), P(ROW, COL))
    return jax.shard_map(step, mesh=split, in_specs=in_specs, out_specs=out_specs, check_vma=False)
```

```python
import functools

import jax
import jax.numpy as jnp
from jax import lax
from jax.experimental import pallas as pl
from jax.experimental.pallas import tpu as pltpu
from jax.sharding import Mesh
from jax.sharding import PartitionSpec as P


TILE = 256
ROW = ("row_0", "row_1")
COL = ("col_0", "col_1")
ALL = ROW + COL
LANES = 128
UNROLL = 33
CHUNKS = 4


def splat(row, lane, k):
    return jnp.broadcast_to(
        jnp.sum(jnp.where(lane == k, row, 0.0), axis=1, keepdims=True), (8, LANES)
    )


def matmul3(a, b):
    return [
        [a[i][0] * b[0][j] + a[i][1] * b[1][j] + a[i][2] * b[2][j] for j in range(3)]
        for i in range(3)
    ]


def phi_column(hess, scale, order):
    inv = 1.0 / 1024.0
    base = [[hess[i][j] * (scale * inv) for j in range(3)] for i in range(3)]
    zero = jnp.zeros((8, LANES), jnp.float32)
    term = base
    cols = [[zero + inv, zero, zero]] + [[zero] * 3 for _ in range(order - 1)]
    total = base
    sums = cols
    for degree in range(2, 11):
        first = [term[i][0] * (inv / degree) for i in range(3)]
        cols = [first] + [[c * (inv / degree) for c in col] for col in cols[:-1]]
        term = [[v * (1.0 / degree) for v in row] for row in matmul3(term, base)]
        total = [[total[i][j] + term[i][j] for j in range(3)] for i in range(3)]
        sums = [[s + c for s, c in zip(sc, cc)] for sc, cc in zip(sums, cols)]
    one, two = inv, 0.5 * inv * inv
    for _ in range(10):
        moved = []
        for n, col in enumerate(sums):
            new = [
                2.0 * col[i]
                + (total[i][0] * col[0] + total[i][1] * col[1] + total[i][2] * col[2])
                for i in range(3)
            ]
            if n >= 1:
                new = [new[i] + sums[n - 1][i] * one for i in range(3)]
            if n >= 2:
                new = [new[i] + sums[n - 2][i] * two for i in range(3)]
            moved.append(new)
        square = matmul3(total, total)
        total = [[2.0 * total[i][j] + square[i][j] for j in range(3)] for i in range(3)]
        sums = moved
        one, two = 2.0 * one, 2.0 * two + one * one
    return sums[-1]


def root(x):
    inv = lax.rsqrt(x)
    inv = inv * (1.5 - 0.5 * (x * inv) * inv)
    return x * inv, inv


def hessenberg(gathered):
    lane = lax.broadcasted_iota(jnp.int32, (8, LANES), 1)
    row = jnp.broadcast_to(jnp.sum(gathered, axis=0, keepdims=True), (8, LANES))
    m = [splat(row, lane, n) for n in range(6)]
    r00, i0 = root(m[0])
    r01, r02, r03 = m[1] * i0, m[2] * i0, m[3] * i0
    r11, i1 = root(jnp.maximum(m[2] - r01 * r01, 1e-9 * m[2]))
    r12, r13 = (m[3] - r01 * r02) * i1, (m[4] - r01 * r03) * i1
    r22, i2 = root(jnp.maximum(m[4] - r02 * r02 - r12 * r12, 1e-9 * m[4]))
    r23 = (m[5] - r02 * r03 - r12 * r13) * i2
    zero = jnp.zeros((8, LANES), jnp.float32)
    j0, j1, j2 = 8.0 * i0, 8.0 * i1, 8.0 * i2
    c0 = [r01 * j0, r11 * j0, zero]
    d0, d1 = 0.125 * c0[0], 0.125 * c0[1]
    c1 = [(r02 - d0 * r01) * j1, (r12 - d1 * r01) * j1, r22 * j1]
    e0, e1, e2 = [0.125 * v for v in c1]
    c2 = [(r03 - d0 * r02 - e0 * r12) * j2, (r13 - d1 * r02 - e1 * r12) * j2, (r23 - e2 * r12) * j2]
    hess = [[c0[i], c1[i], c2[i]] for i in range(3)]
    for i in range(3):
        hess[i][i] = hess[i][i] - 8.0
    return (r00, r01, r02, r12, i0, i1, i2), hess


def on_basis(r, weights, factor):
    r00, r01, r02, r12, i0, i1, i2 = r
    scale = factor * r00
    d2 = weights[2] * i2
    d1 = (weights[1] - r12 * d2) * i1
    d0 = (weights[0] - r01 * d1 - r02 * d2) * i0
    return [d0 * scale, d1 * scale, d2 * scale]


def beside(ref, at, sides):
    tiles = ref.shape[0]
    lane = lax.broadcasted_iota(jnp.int32, (8, LANES), 1)
    mids = [ref[j, pl.ds(at, 8), :] for j in range(tiles)]
    ones = [pltpu.roll(m, 1, 1) for m in mids]
    out = [jnp.where(lane == 0, ones[j - 1], ones[j]) for j in range(tiles)]
    if sides == 2:
        backs = [pltpu.roll(m, LANES - 1, 1) for m in mids]
        out = [o + jnp.where(lane == LANES - 1, backs[(j + 1) % tiles], backs[j]) for j, o in enumerate(out)]
    return out


def sum_row(sums):
    sub = lax.broadcasted_iota(jnp.int32, (8, LANES), 0)
    lane = lax.broadcasted_iota(jnp.int32, (8, LANES), 1)
    rows = jnp.zeros((8, LANES), jnp.float32)
    for n, s in enumerate(sums):
        part = jnp.sum(s, axis=0, keepdims=True)
        rows = jnp.where(sub == n, part, rows)
    values = jnp.sum(rows, axis=1, keepdims=True)
    row = jnp.sum(jnp.where(lane == sub, values, 0.0), axis=0, keepdims=True)
    return jnp.broadcast_to(row, (8, LANES))


def write_row(row, out_ref):
    for i in range(0, out_ref.shape[0], 8):
        out_ref[i : i + 8, :] = row


def band_of(group, bands):
    return jnp.clip((group - 1 + TILE // 8) // (TILE // 8), 0, bands - 1)


def act_of(act_ref, group):
    bands = act_ref.shape[1] // 8
    if isinstance(group, int):
        band = 8 * min(max((group - 1 + TILE // 8) // (TILE // 8), 0), bands - 1)
    else:
        band = pl.multiple_of(8 * band_of(group, bands), 8)
    return [act_ref[j, pl.ds(band, 8), :] for j in range(act_ref.shape[0])]


def over_groups(lo, hi, emit, carry, most=UNROLL):
    unroll = min(most, hi - lo)
    while (hi - lo) % unroll:
        unroll -= 1

    def step(i, c):
        group = lo + i * unroll
        at = pl.multiple_of(8 + 8 * group, 8)
        for u in range(unroll):
            c = emit(group + u, at + 8 * u, c)
        return c

    if hi - lo == unroll:
        for g in range(lo, hi):
            carry = emit(g, 8 + 8 * g, carry)
        return carry
    return lax.fori_loop(0, (hi - lo) // unroll, step, carry)


def is_own(group, groups):
    return not isinstance(group, int) or 0 < group < groups - 1


def add_products(sums, pairs, own):
    out = []
    for s, (a, b) in zip(sums, pairs):
        terms = [x * y for x, y in zip(a[:own], b[:own])]
        while len(terms) > 1:
            terms = [x + y for x, y in zip(terms[::2], terms[1::2])] + terms[len(terms) & ~1 :]
        out.append(s + terms[0])
    return tuple(out)


def no_sums(count):
    return tuple(jnp.zeros((8, LANES), jnp.float32) for _ in range(count))


def power_of(src, dst, coef_ref, act_ref):
    tiles, rows, _ = src.shape
    groups = (rows - 16) // 8

    def emit(group, at, sums):
        side = beside(src, at, 2)
        acts = act_of(act_ref, group)
        here = pl.ds(at, 8)
        mids, outs = [], []
        for j in range(tiles):
            mid = src[j, here, :]
            total = side[j] + (src[j, pl.ds(at - 1, 8), :] + src[j, pl.ds(at + 1, 8), :])
            out = acts[j] * total + coef_ref[j, here, :] * mid
            dst[j, here, :] = out
            mids.append(mid)
            outs.append(out)
        return add_products(sums, ((mids, outs), (outs, outs)), tiles - 1) if is_own(group, groups) else sums

    return emit


def form_of(src, coef_ref):
    tiles = src.shape[0]

    def emit(group, at, sums):
        side = beside(src, at, 1)
        here = pl.ds(at, 8)
        mids, images = [], []
        for j in range(tiles - 1):
            mid = src[j, here, :]
            images.append(0.5 * (side[j] + src[j, pl.ds(at - 1, 8), :]) + coef_ref[j, here, :] * mid)
            mids.append(mid)
        return add_products(sums, ((mids, images),), tiles - 1)

    return emit


def force_of(p_ref, w0, coef_ref, act_ref):
    tiles, rows, _ = p_ref.shape
    groups = (rows - 16) // 8

    def emit(group, at, sums):
        side = beside(p_ref, at, 2)
        acts = act_of(act_ref, group)
        here = pl.ds(at, 8)
        outs = []
        for j in range(tiles):
            mid = p_ref[j, here, :]
            total = side[j] + (p_ref[j, pl.ds(at - 1, 8), :] + p_ref[j, pl.ds(at + 1, 8), :])
            square = mid * mid
            out = acts[j] * (8.0 * total - (28.0 + 4.0 * square) * mid)
            w0[j, here, :] = out
            coef_ref[j, here, :] = acts[j] * (0.5 - 1.5 * square)
            outs.append(out)
        return add_products(sums, ((outs, outs),), tiles - 1) if is_own(group, groups) else sums

    return emit


def rows_of(values):
    sub = lax.broadcasted_iota(jnp.int32, (8, LANES), 0)
    out = jnp.zeros((8, LANES), jnp.float32)
    for k, v in enumerate(values):
        out = jnp.where(sub == k, v, out)
    return out


def row_of(block, k):
    return jnp.broadcast_to(block[k : k + 1], (8, LANES))


def strips_kernel(odd_ref, phase_hbm, mask_hbm, near_ref, far_ref, own_ref, p_ref, mask_ref, sems):
    n, width = phase_hbm.shape
    last = width // LANES - 1
    copies = {}
    for j in (0, last, *range(1, last)):
        source = phase_hbm.at[:, j * LANES : (j + 1) * LANES]
        copies[j] = pltpu.make_async_copy(source, p_ref.at[j, 16 : n + 16, :], sems.at[j])
        copies[j].start()
    mask_copy = pltpu.make_async_copy(mask_hbm, mask_ref, sems.at[last + 1])
    mask_copy.start()
    mask_copy.wait()
    odd = jnp.full((8, LANES), odd_ref[1], jnp.int32) > 0
    odd_n = jnp.full((8, n), odd_ref[1], jnp.int32) > 0
    tiles_r, tiles_c = mask_ref.shape
    mask = [[mask_ref[t, c].astype(jnp.float32) for c in range(tiles_c)] for t in range(tiles_r)]
    own_ref[...] = rows_of([v for row in mask for v in row])
    copies[0].wait()
    copies[last].wait()
    strips = []
    for j, rows, col in ((0, 0, 0), (last, LANES - 8, -1)):
        strip = p_ref[j, 16 : n + 16, :].T[rows : rows + 8, :]
        strips.append((strip, rows_of([row[col] for row in mask])))
    left, right = strips
    for out, a, b in ((near_ref, left, right), (far_ref, right, left)):
        out[:, :n] = jnp.where(odd_n, a[0], b[0])
        out[:, n:] = jnp.where(odd, a[1], b[1])
    for j in range(1, last):
        copies[j].wait()


def corners_kernel(odd_ref, near_in, far_in, p_ref, own_ref, ends_ref, masks_ref, near_ref, far_ref):
    tiles, rows, _ = p_ref.shape
    n, width = rows - 32, LANES * (tiles - 1)
    tiles_r, tiles_c = n // TILE, width // TILE
    odd = jnp.full((8, LANES), odd_ref[1], jnp.int32) > 0
    odd_n = jnp.full((8, n), odd_ref[1], jnp.int32) > 0
    from_left = jnp.where(odd_n, near_in[:, :n], far_in[:, :n])
    from_right = jnp.where(odd_n, far_in[:, :n], near_in[:, :n])
    mask_left = jnp.where(odd, near_in[:, n:], far_in[:, n:])
    mask_right = jnp.where(odd, far_in[:, n:], near_in[:, n:])
    ends_ref[0] = from_right
    ends_ref[1] = from_left
    masks_ref[0] = mask_left
    masks_ref[1] = mask_right
    zeros = jnp.zeros((LANES - 16, LANES), jnp.float32)
    own = own_ref[...]
    odd_row = jnp.full((8, LANES), odd_ref[0], jnp.int32) > 0
    strips = []
    for at, part, row, t in ((16, slice(0, LANES), 0, 0), (n + 8, slice(n - LANES, n), LANES - 8, tiles_r - 1)):
        corner = jnp.concatenate([from_right[:, part], zeros, from_left[:, part]], axis=0).T[row : row + 8, :]
        masks = [row_of(own, t * tiles_c + c) for c in range(tiles_c)]
        masks += [row_of(mask_right, t), row_of(mask_left, t)]
        strips.append([p_ref[j, at : at + 8, :] for j in range(tiles - 1)] + [corner, rows_of(masks)])
    up, down = strips
    for out, a, b in ((near_ref, up, down), (far_ref, down, up)):
        for j in range(tiles + 1):
            out[:, j * LANES : (j + 1) * LANES] = jnp.where(odd_row, a[j], b[j])


def act_cells(act_ref, band, values, right, left):
    tiles = act_ref.shape[0]
    lane = lax.broadcasted_iota(jnp.int32, (8, LANES), 1)
    for j in range(tiles - 1):
        act_ref[j, 8 * band : 8 * band + 8, :] = 0.25 * values[j * LANES // TILE]
    ends = jnp.where(lane < 8, right, jnp.where(lane >= LANES - 8, left, 0.0))
    act_ref[tiles - 1, 8 * band : 8 * band + 8, :] = 0.25 * ends


def first_passes(p_ref, w0, w1, w2, coef_ref, act_ref):
    return (
        (force_of(p_ref, w0, coef_ref, act_ref), 1),
        (power_of(w0, w1, coef_ref, act_ref), 2),
        (power_of(w1, w2, coef_ref, act_ref), 2),
        (form_of(w2, coef_ref), 1),
    )


def inner_kernel(ends_ref, masks_ref, own_ref, p_in, p_ref, w0, w1, w2, coef_ref, act_ref, sums_ref):
    tiles, rows, _ = p_ref.shape
    n, width = rows - 32, LANES * (tiles - 1)
    groups = n // 8 + 2
    tiles_r, tiles_c = n // TILE, width // TILE
    for t in range(tiles_r):
        values = [row_of(own_ref[...], t * tiles_c + c) for c in range(tiles_c)]
        act_cells(act_ref, t + 1, values, row_of(masks_ref[1], t), row_of(masks_ref[0], t))
    zeros = jnp.zeros((LANES - 16, n), jnp.float32)
    p_ref[tiles - 1, 16 : n + 16, :] = jnp.concatenate([ends_ref[0], zeros, ends_ref[1]], axis=0).T
    sums = []
    for k, (emit, count) in enumerate(first_passes(p_ref, w0, w1, w2, coef_ref, act_ref)):
        sums += over_groups(2 + k, groups - 2 - k, emit, no_sums(count))
    sums_ref[...] = sum_row(sums)


def outer_kernel(
    odd_ref, near_in, far_in, inner_ref, p_in, w0_in, w1_in, w2_in, coef_in, act_in,
    p_ref, w0, w1, w2, coef_ref, act_ref, sums_ref,
):
    tiles, rows, _ = p_ref.shape
    n = rows - 32
    groups = n // 8 + 2
    width = LANES * (tiles - 1)
    tiles_r, tiles_c = n // TILE, width // TILE
    odd = jnp.full((8, LANES), odd_ref[0], jnp.int32) > 0
    near = [near_in[:, j * LANES : (j + 1) * LANES] for j in range(tiles + 1)]
    far = [far_in[:, j * LANES : (j + 1) * LANES] for j in range(tiles + 1)]
    *up, up_masks = [jnp.where(odd, a, b) for a, b in zip(near, far)]
    *down, down_masks = [jnp.where(odd, b, a) for a, b in zip(near, far)]
    for t, masks in ((0, up_masks), (tiles_r + 1, down_masks)):
        values = [row_of(masks, c) for c in range(tiles_c + 2)]
        act_cells(act_ref, t, values[:tiles_c], values[tiles_c], values[tiles_c + 1])
    blank = jnp.zeros((8, LANES), jnp.float32)
    for ref in (p_ref, w0, w1, w2):
        for j in range(tiles):
            ref[j, 0:8, :] = blank
            ref[j, n + 24 : n + 32, :] = blank
    for at, strip in ((8, up), (n + 16, down)):
        for j in range(tiles):
            p_ref[j, at : at + 8, :] = strip[j]
    sums = []
    for k, (emit, count) in enumerate(first_passes(p_ref, w0, w1, w2, coef_ref, act_ref)):
        own = k == 3
        part = no_sums(count)
        part = over_groups(1 if own else 0, 2 + k, emit, part)
        sums += over_groups(groups - 2 - k, groups - 1 if own else groups, emit, part)
    write_row(sum_row(sums) + inner_ref[...], sums_ref)


def second_kernel(
    gathered_ref, p_ref, w0, w1, w2, coef_ref, act_ref,
    section_hbm, base_ref, v0, v1, v2, sums_ref, section_ref, sem,
):
    tiles, rows, _ = p_ref.shape
    groups = (rows - 16) // 8
    r, hess = hessenberg(gathered_ref[...])
    scale = jnp.where(lax.broadcasted_iota(jnp.int32, (8, LANES), 0) < 4, 0.5, 1.0)
    coefs = on_basis(r, phi_column(hess, scale, 1), scale)
    a = [jnp.broadcast_to(c[0:1], (8, LANES)) for c in coefs]
    f = [jnp.broadcast_to(c[7:8], (8, LANES)) for c in coefs]
    blank = jnp.zeros((8, LANES), jnp.float32)
    for ref in (v0, v1, v2):
        for j in range(tiles):
            ref[j, 0:8, :] = blank
            ref[j, rows - 8 : rows, :] = blank

    def start(group, at, sums):
        acts = act_of(act_ref, group)
        here = pl.ds(at, 8)
        own = is_own(group, groups)
        outs = []
        for j in range(tiles):
            ws = [ref[j, here, :] for ref in (w0, w1, w2)]
            phase = p_ref[j, here, :]
            shift = a[0] * ws[0] + a[1] * ws[1] + a[2] * ws[2]
            out = (acts[j] * (shift * shift)) * (shift + 3.0 * phase)
            v0[j, here, :] = out
            outs.append(out)
            if own and j < tiles - 1:
                to = pl.ds(at - 16 if isinstance(at, int) else pl.multiple_of(at - 16, 8), 8)
                cols = slice(j * LANES, (j + 1) * LANES)
                section_ref[to, cols] = phase + shift
                base_ref[to, cols] = phase + (f[0] * ws[0] + f[1] * ws[1] + f[2] * ws[2])
        return add_products(sums, ((outs, outs),), tiles - 1) if own else sums

    def sides(emit, count, most):
        part = over_groups(0, 1, emit, no_sums(count))
        part = over_groups(1, groups - 1, emit, part, most)
        return over_groups(groups - 1, groups, emit, part)

    power = power_of(v0, v1, coef_ref, act_ref)

    def fused(group, at, c):
        return start(group, at, c[0]), power(group - 2, at - 16, c[1])

    part = no_sums(1), no_sums(2)
    part = over_groups(0, 3, start, part[0]), over_groups(0, 1, power, part[1])
    part = over_groups(3, groups - 1, fused, part)
    part = over_groups(groups - 1, groups, start, part[0]), part[1]
    copy = pltpu.make_async_copy(section_ref, section_hbm, sem)
    copy.start()
    sums = [*part[0], *over_groups(groups - 3, groups, power, part[1])]
    sums += sides(power_of(v1, v2, coef_ref, act_ref), 2, UNROLL)
    sums += over_groups(1, groups - 1, form_of(v2, coef_ref), no_sums(1))
    write_row(sum_row(sums), sums_ref)
    copy.wait()


def third_kernel(gathered_ref, base_ref, v0, v1, v2, updated_hbm, updated_ref, sems):
    n, width = base_ref.shape
    r, hess = hessenberg(gathered_ref[...])
    d = on_basis(r, phi_column(hess, 1.0, 3), -4.0 * 32.0)

    def emit(group, at, c):
        here = pl.ds(at, 8)
        to = pl.ds(pl.multiple_of(at - 16, 8), 8)
        for j in range(width // LANES):
            cols = slice(j * LANES, (j + 1) * LANES)
            updated_ref[to, cols] = base_ref[to, cols] + (
                d[0] * v0[j, here, :] + d[1] * v1[j, here, :] + d[2] * v2[j, here, :]
            )
        return c

    copies = []
    chunk = n // CHUNKS
    for k in range(CHUNKS):
        over_groups(1 + k * chunk // 8, 1 + (k + 1) * chunk // 8, emit, 0, 4)
        part = pl.ds(k * chunk, chunk)
        copies.append(pltpu.make_async_copy(updated_ref.at[part, :], updated_hbm.at[part, :], sems.at[k]))
        copies[-1].start()
    for copy in copies:
        copy.wait()


def params(mib):
    return pltpu.CompilerParams(vmem_limit_bytes=mib << 20)


VM = pl.BlockSpec(memory_space=pltpu.VMEM)
SM = pl.BlockSpec(memory_space=pltpu.SMEM)
HB = pl.BlockSpec(memory_space=pltpu.HBM)


def in_pairs(near, far, axis):
    size = lax.axis_size(axis)
    odd = [(i, ((i + 1) ^ 1) - 1) for i in range(1, size - 1)]
    far = lax.ppermute(far, axis, odd)
    near = lax.ppermute(near, axis, [(i, i ^ 1) for i in range(size)])
    return near, far


def total(sums):
    size = sums.shape[0]
    sent = lax.all_to_all(sums.reshape(size, 1, LANES), ALL[::-1], 0, 0, tiled=True)
    return sent.reshape(size, LANES)


def step(phase, tile_mask):
    n, width = phase.shape
    f32 = jnp.float32
    sd = jax.ShapeDtypeStruct
    odd = jnp.stack([lax.axis_index(ROW) % 2, lax.axis_index(COL) % 2]).astype(jnp.int32)
    tiles = width // LANES + 1
    ext = sd((tiles, n + 32, LANES), f32)
    act = sd((tiles, 8 * (n // TILE + 2), LANES), f32)
    edge = sd((8, width + 2 * LANES), f32)
    hbm = functools.partial(pltpu.with_memory_space_constraint, memory_space=pltpu.HBM)
    near, far, own_mask, p = pl.pallas_call(
        strips_kernel,
        in_specs=[SM, HB, HB],
        out_specs=[VM] * 4,
        out_shape=[sd((8, n + LANES), f32)] * 2 + [sd((8, LANES), f32), ext],
        scratch_shapes=[pltpu.SMEM(tile_mask.shape, jnp.int32), pltpu.SemaphoreType.DMA((tiles,))],
        compiler_params=params(6),
        name="strips",
    )(odd, hbm(phase), hbm(tile_mask))
    near, far = in_pairs(near, far, COL)
    ends, masks, near, far = pl.pallas_call(
        corners_kernel,
        in_specs=[SM] + [VM] * 4,
        out_specs=[VM] * 4,
        out_shape=[sd((2, 8, n), f32), sd((2, 8, LANES), f32), edge, edge],
        compiler_params=params(6),
        name="corners",
    )(odd, near, far, p, own_mask)
    near, far = in_pairs(near, far, ROW)
    devices = 1
    for axis in ALL:
        devices *= lax.axis_size(axis)
    sums = sd((devices, LANES), f32)
    fields = [ext] * 5 + [act]
    *held, part = pl.pallas_call(
        inner_kernel,
        in_specs=[VM] * 4,
        out_specs=[VM] * 7,
        out_shape=fields + [sd((8, LANES), f32)],
        input_output_aliases={3: 0},
        compiler_params=params(14),
        name="inner",
    )(ends, masks, own_mask, p)
    *held, part = pl.pallas_call(
        outer_kernel,
        in_specs=[SM] + [VM] * 9,
        out_specs=[VM] * 7,
        out_shape=fields + [sums],
        input_output_aliases={4 + i: i for i in range(6)},
        compiler_params=params(14),
        name="outer",
    )(odd, near, far, part, *held)
    p, w0, w1, w2, coef, act = held
    gathered = total(part)
    own = sd((n, width), f32)
    section, base, v0, v1, v2, part = pl.pallas_call(
        second_kernel,
        in_specs=[VM] * 7,
        out_specs=[HB] + [VM] * 5,
        out_shape=[own, own, ext, ext, ext, sums],
        scratch_shapes=[pltpu.VMEM((n, width), f32), pltpu.SemaphoreType.DMA(())],
        compiler_params=params(20),
        name="second",
    )(gathered, p, w0, w1, w2, coef, act)
    updated = pl.pallas_call(
        third_kernel,
        in_specs=[VM] * 5,
        out_specs=HB,
        out_shape=own,
        scratch_shapes=[pltpu.VMEM((n, width), f32), pltpu.SemaphoreType.DMA((CHUNKS,))],
        compiler_params=params(10),
        name="third",
    )(total(part), base, v0, v1, v2)
    return updated, section


def solution(mesh):
    split = Mesh(mesh.devices.reshape(4, 4, 4, 2), ALL)
    in_specs = (P(ROW, COL), P(ROW, COL))
    out_specs = (P(ROW, COL), P(ROW, COL))
    return jax.shard_map(step, mesh=split, in_specs=in_specs, out_specs=out_specs, check_vma=False)
```
